8 devices in a mesh: mat: 1 (over z), dp: 8 (over y, x, core).
Axes of the slice: x: 2, y: 2, z: 1, core: 2. Of those that a mesh axis runs over, the one named last changes fastest.
Arguments:
- a_mat: bfloat16 [3072, 32768], P('mat', 'dp')
Outputs:
- output: float32 [8, 5, 384, 384], P(('mat', 'dp'))
All inputs are finite; a program needn't handle non-finite values.
Results may differ from the reference program's by a relative error of at most 0.001.
Values are sent between devices in bfloat16 or wider.
A program may use at most 1 GiB of HBM per device.

```python
import jax
import jax.numpy as jnp
from jax import lax

GRAM_ORDER = 3072
COLS_DEV = 4096
GROUPS = 8
MIX_RANK = 8

BLOCK = GRAM_ORDER // GROUPS
SLOTS = GROUPS // 2 + 1
WIDTH = COLS_DEV * GROUPS


def pair_table():
    half = GROUPS // 2
    hi_list = []
    lo_list = []
    for dev_index in range(GROUPS):
        for slot in range(SLOTS):
            other_id = (dev_index - slot) % GROUPS
            if slot < half or dev_index < half:
                hi_list.append(max(dev_index, other_id))
                lo_list.append(min(dev_index, other_id))
            else:
                hi_list.append(-1)
                lo_list.append(-1)
    return jnp.array(hi_list, dtype=jnp.int32), jnp.array(lo_list, dtype=jnp.int32)


def setup_inputs(seed: int = 0, part: int = 0) -> dict:
    key = jax.random.fold_in(jax.random.key(seed), part)
    key_mix, key_src, key_gain = jax.random.split(key, 3)
    mixers = jax.random.normal(key_mix, (GROUPS, GRAM_ORDER, MIX_RANK), jnp.float32) * MIX_RANK ** -0.5
    sources = jax.random.normal(key_src, (GROUPS, MIX_RANK, COLS_DEV), jnp.float32)
    block_gain = jax.random.uniform(key_gain, (GROUPS,), jnp.float32, minval=0.7, maxval=1.4)
    row_gain = jnp.repeat(block_gain, BLOCK)
    mixed = jnp.einsum('snr,srk->nsk', mixers, sources).reshape(GRAM_ORDER, WIDTH)
    scale = (MIX_RANK ** 0.5 / (COLS_DEV * GROUPS ** 0.5)) ** 0.5
    a_mat = mixed * (row_gain[:, None] * scale)
    return {'a_mat': a_mat.astype(jnp.bfloat16)}


def reference(a_mat):
    hi_ids, lo_ids = pair_table()

    def one_block(pair_ids):
        hi_id, lo_id = pair_ids
        hi_rows = lax.dynamic_slice_in_dim(a_mat, jnp.maximum(hi_id, 0) * BLOCK, BLOCK, axis=0)
        lo_rows = lax.dynamic_slice_in_dim(a_mat, jnp.maximum(lo_id, 0) * BLOCK, BLOCK, axis=0)
        block_prod = jnp.dot(hi_rows, lo_rows.T, preferred_element_type=jnp.float32)
        return jnp.where(hi_id >= 0, block_prod, 0.0)

    blocks = lax.map(one_block, (hi_ids, lo_ids))
    return blocks.reshape(GROUPS, SLOTS, BLOCK, BLOCK)
```

```python
import functools

import jax
import jax.numpy as jnp
from jax import lax
from jax.experimental import pallas as pl
from jax.experimental.pallas import tpu as pltpu
from jax.sharding import PartitionSpec as P

MESH = pl.DeviceIdType.MESH
BLK = 384
STRIP = 128
GROUPS = 8
SLOTS = 5
DIAG, ALONG_X, ALONG_Y, HERE = range(4)
STEPS = 20


def gram_kernel(a_hbm, out_ref, a_buf, acc, stage, from_x, from_y, relay_x, relay_y,
                load_sem, stage_sem, pair_sem, send_sem, fx_sem, fy_sem, rx_sem, ry_sem):
    me = lax.axis_index('dp')
    core = lax.rem(me, 2)
    x = lax.rem(me // 2, 2)
    y = me // 4

    def device(xx, yy, kk):
        return (yy * 2 + xx) * 2 + kk

    pair = device(x, y, 1 - core)
    nbr_x = device(1 - x, y, core)
    nbr_y = device(x, 1 - y, core)

    barrier = pltpu.get_barrier_semaphore()
    for other in (pair, nbr_x, nbr_y):
        pl.semaphore_signal(barrier, inc=1, device_id={'dp': other}, device_id_type=MESH)

    far = device(1 - x, 1 - y, 0)

    def load(n):
        if isinstance(n, int) and n < 2:
            row = far + (1 - core if n == 0 else core)
        else:
            row = lax.rem(far + 1 - n + GROUPS, GROUPS)
        rows = pl.ds(pl.multiple_of(row * BLK, BLK), BLK)
        return pltpu.make_async_copy(a_hbm.at[rows, :], a_buf.at[rows, :], load_sem.at[n])

    for n in range(GROUPS):
        load(n).start()

    def step_task(step):
        mid = step - SLOTS
        in_mid = jnp.logical_and(mid >= 0, mid < 2 * SLOTS)
        rel = jnp.where(step < SLOTS, DIAG, jnp.where(in_mid, ALONG_X + lax.rem(mid + 2 * SLOTS, 2), HERE))
        slot = jnp.where(step < SLOTS, step, jnp.where(in_mid, mid // 2, step - 3 * SLOTS))
        return rel, slot

    def dest_xy(rel):
        flip_x = jnp.where(rel <= ALONG_X, 1, 0)
        flip_y = jnp.where(lax.rem(rel, 2) == 0, 1, 0)
        xx = x + flip_x - 2 * flip_x * x
        yy = y + flip_y - 2 * flip_y * y
        return xx, yy

    def exists(rel, slot):
        _, yy = dest_xy(rel)
        return jnp.logical_or(slot < SLOTS - 1, yy == 0)

    def product(rel, slot, kk):
        xx, yy = dest_xy(rel)
        p = device(xx, yy, kk)
        q = lax.rem(p - slot + GROUPS, GROUPS)
        hi = pl.multiple_of(jnp.maximum(p, q) * BLK, BLK)
        lo = pl.multiple_of(jnp.minimum(p, q) * BLK, BLK)
        return lax.dot_general(a_buf[pl.ds(hi, BLK), :], a_buf[pl.ds(lo, BLK), :],
                               (((1,), (1,)), ((), ())), preferred_element_type=jnp.float32)

    def pair_copy(step):
        rel, slot = step_task(step)
        return pltpu.make_async_remote_copy(
            src_ref=stage.at[lax.rem(step, 2)], dst_ref=acc.at[rel, slot],
            send_sem=stage_sem.at[lax.rem(step, 2)], recv_sem=pair_sem.at[rel, slot],
            device_id={'dp': pair}, device_id_type=MESH)

    def pair_step(step):
        rel, slot = step_task(step)

        @pl.when(exists(rel, slot))
        def _():
            stage[lax.rem(step, 2)] = product(rel, slot, 1 - core)
            pair_copy(step).start()

    def by_y(ordinal, dest_y):
        long_n, long_o = 5 + core, 4 - 2 * core
        short = ((ordinal + 1) * 7) // 11 - (ordinal * 7) // 11
        full = ((ordinal + 1) * long_n + long_o) // 14 - (ordinal * long_n + long_o) // 14
        return jnp.where(dest_y == 1, short, full) == 1

    def strip(m):
        return pl.ds(m * STRIP, STRIP)

    def ordinal(slot, m):
        return jnp.where(slot == 0, m // 2, 3 * slot - 1 + m)

    def sent(slot, m):
        return slot >= (1 if m == 1 else 0)

    def far_send(slot, m, along_y):
        return pltpu.make_async_remote_copy(
            src_ref=acc.at[DIAG, slot, strip(m)],
            dst_ref=(relay_x if along_y else relay_y).at[slot, strip(m)],
            send_sem=send_sem.at[DIAG, slot, m],
            recv_sem=(rx_sem if along_y else ry_sem).at[slot, m],
            device_id={'dp': nbr_y if along_y else nbr_x}, device_id_type=MESH)

    def near_send(rel, slot, m):
        along_y = rel == ALONG_Y
        return pltpu.make_async_remote_copy(
            src_ref=acc.at[rel, slot, strip(m)],
            dst_ref=(from_y if along_y else from_x).at[slot, strip(m)],
            send_sem=send_sem.at[rel, slot, m],
            recv_sem=(fy_sem if along_y else fx_sem).at[slot, m],
            device_id={'dp': nbr_y if along_y else nbr_x}, device_id_type=MESH)

    def own_step(step):
        rel, slot = step_task(step)

        @pl.when(exists(rel, slot))
        def _():
            pair_copy(step).wait_recv()
            acc[rel, slot] = acc[rel, slot] + product(rel, slot, core)

            @pl.when(slot == 0)
            def _():
                acc[rel, slot, 0:STRIP, STRIP:] = acc[rel, slot, STRIP:2 * STRIP, :2 * STRIP]

            for m in range(3):
                @pl.when(jnp.logical_and(rel == DIAG, sent(slot, m)))
                def _(m=m):
                    along_y = by_y(ordinal(slot, m), 1 - y)

                    @pl.when(along_y)
                    def _():
                        far_send(slot, m, True).start()

                    @pl.when(jnp.logical_not(along_y))
                    def _():
                        far_send(slot, m, False).start()

                @pl.when(jnp.logical_and(rel == ALONG_X, sent(slot, m)))
                def _(m=m):
                    @pl.when(by_y(ordinal(slot, m), y))
                    def _():
                        far_send(slot, m, True).wait_recv()
                        acc[ALONG_X, slot, strip(m)] = acc[ALONG_X, slot, strip(m)] + relay_x[slot, strip(m)]

                    near_send(ALONG_X, slot, m).start()

                @pl.when(jnp.logical_and(rel == ALONG_Y, sent(slot, m)))
                def _(m=m):
                    @pl.when(jnp.logical_not(by_y(ordinal(slot, m), 1 - y)))
                    def _():
                        far_send(slot, m, False).wait_recv()
                        acc[ALONG_Y, slot, strip(m)] = acc[ALONG_Y, slot, strip(m)] + relay_y[slot, strip(m)]

                    near_send(ALONG_Y, slot, m).start()

    load(0).wait()
    first = product(DIAG, 0, 1 - core)
    stage[0] = first
    pl.semaphore_wait(barrier, 3)
    pair_copy(0).start()
    load(1).wait()
    own_step(0)
    load(2).wait()
    pair_step(1)

    def body(step, carry):
        @pl.when(step < SLOTS)
        def _():
            load(step + 2).wait()

        @pl.when(step == SLOTS - 1)
        def _():
            load(GROUPS - 1).wait()

        @pl.when(step < STEPS - 1)
        def _():
            @pl.when(exists(*step_task(step - 1)))
            def _():
                pair_copy(step - 1).wait_send()

            pair_step(step + 1)

        own_step(step)
        return carry

    lax.fori_loop(1, STEPS, body, 0)

    for step in (STEPS - 2, STEPS - 1):
        @pl.when(exists(*step_task(step)))
        def _(step=step):
            pair_copy(step).wait_send()

    for slot in range(SLOTS):
        @pl.when(exists(HERE, slot))
        def _(slot=slot):
            for m in range(3):
                if slot == 0 and m == 1:
                    continue
                near_send(ALONG_X, slot, m).wait_recv()
                near_send(ALONG_Y, slot, m).wait_recv()
                total = acc[HERE, slot, strip(m)] + from_x[slot, strip(m)] + from_y[slot, strip(m)]
                if slot:
                    out_ref[0, slot, strip(m)] = total
                elif m == 0:
                    out_ref[0, 0, 0:STRIP, 0:STRIP] = total[:, 0:STRIP]
                    out_ref[0, 0, STRIP:2 * STRIP, 0:2 * STRIP] = total[:, STRIP:]
                    out_ref[0, 0, 0:STRIP, STRIP:2 * STRIP] = total[:, STRIP:2 * STRIP].T
                else:
                    out_ref[0, 0, strip(2)] = total
                    out_ref[0, 0, 0:STRIP, 2 * STRIP:] = total[:, 0:STRIP].T
                    out_ref[0, 0, STRIP:2 * STRIP, 2 * STRIP:] = total[:, STRIP:2 * STRIP].T

        if slot == SLOTS - 1:
            @pl.when(jnp.logical_not(exists(HERE, slot)))
            def _(slot=slot):
                out_ref[0, slot] = jnp.zeros((BLK, BLK), jnp.float32)

    for rel in (DIAG, ALONG_X, ALONG_Y):
        for slot in range(SLOTS):
            @pl.when(exists(rel, slot))
            def _(rel=rel, slot=slot):
                for m in range(3):
                    if slot == 0 and m == 1:
                        continue
                    if rel == DIAG:
                        far_send(slot, m, True).wait_send()
                    else:
                        near_send(rel, slot, m).wait_send()


def solution(mesh):
    def local_gram(a_local):
        block = (SLOTS, BLK, BLK)
        dma = pltpu.SemaphoreType.DMA
        return pl.pallas_call(
            gram_kernel,
            out_shape=jax.ShapeDtypeStruct((1,) + block, jnp.float32),
            in_specs=[pl.BlockSpec(memory_space=pl.ANY)],
            out_specs=pl.BlockSpec(memory_space=pltpu.VMEM),
            scratch_shapes=[
                pltpu.VMEM(a_local.shape, a_local.dtype),
                pltpu.VMEM((4,) + block, jnp.float32),
                pltpu.VMEM((2, BLK, BLK), jnp.float32),
                pltpu.VMEM(block, jnp.float32),
                pltpu.VMEM(block, jnp.float32),
                pltpu.VMEM(block, jnp.float32),
                pltpu.VMEM(block, jnp.float32),
                dma((GROUPS,)),
                dma((2,)),
                dma((4, SLOTS)),
                dma((3, SLOTS, 3)),
                dma((SLOTS, 3)),
                dma((SLOTS, 3)),
                dma((SLOTS, 3)),
                dma((SLOTS, 3)),
            ],
            compiler_params=pltpu.CompilerParams(
                collective_id=0, has_side_effects=True, vmem_limit_bytes=67043328),
        )(a_local)

    return jax.shard_map(local_gram, mesh=mesh, in_specs=(P('mat', 'dp'),), out_specs=P(('mat', 'dp')), check_vma=False)
```

```python
import functools

import jax
import jax.numpy as jnp
from jax import lax
from jax.experimental import pallas as pl
from jax.experimental.pallas import tpu as pltpu
from jax.sharding import PartitionSpec as P

MESH = pl.DeviceIdType.MESH
BLK = 384
STRIP = 128
GROUPS = 8
SLOTS = 5
DIAG, ALONG_X, ALONG_Y, HERE = range(4)
STEPS = 20


def pack_symmetric(ref):
    row = lax.broadcasted_iota(jnp.int32, (STRIP, STRIP), 0)
    col = lax.broadcasted_iota(jnp.int32, (STRIP, STRIP), 1)
    s11 = ref[STRIP:2 * STRIP, STRIP:2 * STRIP]
    main = jnp.sum(jnp.where(row == col, s11, 0.0), axis=0, keepdims=True)
    ref[0:STRIP, 0:STRIP] = jnp.where(row >= col, ref[0:STRIP, 0:STRIP], s11)
    ref[0:STRIP, STRIP:2 * STRIP] = ref[STRIP:2 * STRIP, 0:STRIP]
    ref[0:STRIP, 2 * STRIP:] = ref[2 * STRIP:, 0:STRIP]
    ref[STRIP:2 * STRIP, 0:STRIP] = ref[2 * STRIP:, STRIP:2 * STRIP]
    ref[STRIP:2 * STRIP, STRIP:2 * STRIP] = jnp.where(
        row >= col, ref[2 * STRIP:, 2 * STRIP:], jnp.where(row == 0, main, s11[0:1, 0:1]))


def unpack_symmetric(ref, top, low):
    row = lax.broadcasted_iota(jnp.int32, (STRIP, STRIP), 0)
    col = lax.broadcasted_iota(jnp.int32, (STRIP, STRIP), 1)
    both, s10, s20 = top[:, 0:STRIP], top[:, STRIP:2 * STRIP], top[:, 2 * STRIP:]
    s21, last = low[:, 0:STRIP], low[:, STRIP:]
    both_t, last_t = both.T, last.T
    main = jnp.where(col[0:1] == 0, last[1:2, STRIP - 1:STRIP], last[0:1, :])
    ref[0:STRIP, 0:STRIP] = jnp.where(row >= col, both, both_t)
    ref[STRIP:2 * STRIP, STRIP:2 * STRIP] = jnp.where(row == col, main, jnp.where(row < col, both, both_t))
    ref[2 * STRIP:, 2 * STRIP:] = jnp.where(row >= col, last, last_t)
    ref[STRIP:2 * STRIP, 0:STRIP] = s10
    ref[0:STRIP, STRIP:2 * STRIP] = s10.T
    ref[2 * STRIP:, 0:STRIP] = s20
    ref[0:STRIP, 2 * STRIP:] = s20.T
    ref[2 * STRIP:, STRIP:2 * STRIP] = s21
    ref[STRIP:2 * STRIP, 2 * STRIP:] = s21.T


def gram_kernel(a_hbm, out_ref, a_buf, acc, stage, mine, from_x, from_y, relay_x, relay_y,
                load_sem, stage_sem, pair_sem, send_sem, fx_sem, fy_sem, rx_sem, ry_sem):
    me = lax.axis_index('dp')
    core = lax.rem(me, 2)
    x = lax.rem(me // 2, 2)
    y = me // 4
    half = a_buf.shape[1] // 2

    def device(xx, yy, kk):
        return (yy * 2 + xx) * 2 + kk

    pair = device(x, y, 1 - core)
    nbr_x = device(1 - x, y, core)
    nbr_y = device(x, 1 - y, core)

    barrier = pltpu.get_barrier_semaphore()
    for other in (pair, nbr_x, nbr_y):
        pl.semaphore_signal(barrier, inc=1, device_id={'dp': other}, device_id_type=MESH)

    far = device(1 - x, 1 - y, 0)

    def load(n, part=None):
        if isinstance(n, int) and n < 2:
            row = far + (1 - core if n == 0 else core)
        else:
            row = lax.rem(far + 1 - n + GROUPS, GROUPS)
        rows = pl.ds(pl.multiple_of(row * BLK, BLK), BLK)
        if part is None:
            return pltpu.make_async_copy(a_hbm.at[rows, :], a_buf.at[rows, :], load_sem.at[n])
        cols = pl.ds(part * half, half)
        return pltpu.make_async_copy(a_hbm.at[rows, cols], a_buf.at[rows, cols], load_sem.at[GROUPS * part])

    load(0, 0).start()
    load(0, 1).start()
    for n in range(1, GROUPS):
        load(n).start()

    near_first = ALONG_X + y
    near_second = ALONG_Y - y

    def step_task(step):
        mid = step - SLOTS
        in_mid = jnp.logical_and(mid >= 0, mid < 2 * SLOTS)
        near = jnp.where(lax.rem(mid + 2 * SLOTS, 2) == 0, near_first, near_second)
        rel = jnp.where(step < SLOTS, DIAG, jnp.where(in_mid, near, HERE))
        slot = jnp.where(step < SLOTS, step, jnp.where(in_mid, mid // 2, step - 3 * SLOTS))
        return rel, slot

    def dest_xy(rel):
        flip_x = jnp.where(rel <= ALONG_X, 1, 0)
        flip_y = jnp.where(lax.rem(rel, 2) == 0, 1, 0)
        xx = x + flip_x - 2 * flip_x * x
        yy = y + flip_y - 2 * flip_y * y
        return xx, yy

    def exists(rel, slot):
        _, yy = dest_xy(rel)
        return jnp.logical_or(slot < SLOTS - 1, yy == 0)

    def dot(lo, lo_rows, hi, hi_rows, cols=slice(None)):
        return lax.dot_general(a_buf[pl.ds(lo, lo_rows), cols], a_buf[pl.ds(hi, hi_rows), cols],
                               (((1,), (1,)), ((), ())), preferred_element_type=jnp.float32)

    def product(rel, slot, kk):
        xx, yy = dest_xy(rel)
        p = device(xx, yy, kk)
        q = lax.rem(p - slot + GROUPS, GROUPS)
        hi = pl.multiple_of(jnp.maximum(p, q) * BLK, BLK)
        lo = pl.multiple_of(jnp.minimum(p, q) * BLK, BLK)
        return dot(hi, BLK, lo, BLK)

    def pair_copy(step, rows=BLK):
        rel, slot = step_task(step)
        rows = pl.ds(0, rows)
        return pltpu.make_async_remote_copy(
            src_ref=stage.at[lax.rem(step, 2), rows], dst_ref=acc.at[rel, slot, rows],
            send_sem=stage_sem.at[lax.rem(step, 2)], recv_sem=pair_sem.at[rel, slot],
            device_id={'dp': pair}, device_id_type=MESH)

    def by_y(ordinal, dest_y):
        later = ordinal - 2
        long_n, long_o = 4 + core, 8 - core
        short = (later * 2 + 3) // 3 - (later * 2 + 1) // 3
        full = ((later + 1) * long_n + long_o) // 12 - (later * long_n + long_o) // 12
        rest = jnp.where(dest_y == 1, short, full)
        return jnp.where(ordinal < 2, lax.rem(ordinal + core, 2), rest) == 1

    def piece(ref, m, first):
        rows = pl.ds(m * STRIP, STRIP)
        if first and m == 1:
            return ref.at[rows, pl.ds(0, 2 * STRIP)]
        return ref.at[rows, :]

    def pieces(first):
        return range(2 if first else 3)

    def ordinal(slot, m, first):
        return m if first else 3 * slot - 1 + m

    def far_send(slot, m, first, along_y):
        return pltpu.make_async_remote_copy(
            src_ref=piece(acc.at[DIAG, slot], m, first),
            dst_ref=piece((relay_x if along_y else relay_y).at[slot], m, first),
            send_sem=send_sem.at[DIAG, slot, m],
            recv_sem=(rx_sem if along_y else ry_sem).at[slot, m],
            device_id={'dp': nbr_y if along_y else nbr_x}, device_id_type=MESH)

    def near_send(rel, slot, m, first):
        along_y = rel == ALONG_Y
        return pltpu.make_async_remote_copy(
            src_ref=piece(acc.at[rel, slot], m, first),
            dst_ref=piece((from_y if along_y else from_x).at[slot], m, first),
            send_sem=send_sem.at[rel, slot, m],
            recv_sem=(fy_sem if along_y else fx_sem).at[slot, m],
            device_id={'dp': nbr_y if along_y else nbr_x}, device_id_type=MESH)

    def finish(rel, slot, first, only_far=False):
        for m in pieces(first):
            block = piece(acc.at[rel, slot], m, first)
            block[...] = block[...] + piece(mine, m, first)[...]

            def send_far(m=m):
                along_y = by_y(ordinal(slot, m, first), 1 - y)

                @pl.when(along_y)
                def _():
                    far_send(slot, m, first, True).start()

                @pl.when(jnp.logical_not(along_y))
                def _():
                    far_send(slot, m, first, False).start()

            if only_far:
                send_far()
                continue
            pl.when(rel == DIAG)(send_far)

            @pl.when(rel == ALONG_X)
            def _(m=m):
                @pl.when(by_y(ordinal(slot, m, first), y))
                def _():
                    far_send(slot, m, first, True).wait_recv()
                    total = piece(acc.at[ALONG_X, slot], m, first)
                    total[...] = total[...] + piece(relay_x.at[slot], m, first)[...]

                near_send(ALONG_X, slot, m, first).start()

            @pl.when(rel == ALONG_Y)
            def _(m=m):
                @pl.when(jnp.logical_not(by_y(ordinal(slot, m, first), 1 - y)))
                def _():
                    far_send(slot, m, first, False).wait_recv()
                    total = piece(acc.at[ALONG_Y, slot], m, first)
                    total[...] = total[...] + piece(relay_y.at[slot], m, first)[...]

                near_send(ALONG_Y, slot, m, first).start()

    def first_product(ref, kk, halves):
        row = pl.multiple_of((far + kk) * BLK, BLK)
        for h in range(halves):
            cols = pl.ds(h * half, half) if halves > 1 else slice(None)
            if halves > 1:
                load(0, h).wait()
            left = dot(row, BLK, row, 2 * STRIP, cols)
            corner = dot(row + 2 * STRIP, STRIP, row + 2 * STRIP, STRIP, cols)
            if h:
                left = ref[:, 0:2 * STRIP] + left
                corner = ref[2 * STRIP:, 2 * STRIP:] + corner
            ref[:, 0:2 * STRIP] = left
            ref[2 * STRIP:, 2 * STRIP:] = corner
        pack_symmetric(ref)

    first_product(stage.at[0], 1 - core, 2)
    pl.semaphore_wait(barrier, 3)
    pair_copy(0, 2 * STRIP).start()
    load(1).wait()
    first_product(mine, core, 1)
    pair_copy(0, 2 * STRIP).wait_recv()
    finish(DIAG, 0, True, only_far=True)

    def body(step, carry):
        @pl.when(step < SLOTS + 1)
        def _():
            load(step + 1).wait()

        @pl.when(step == SLOTS)
        def _():
            load(GROUPS - 1).wait()

        rel, slot = step_task(step)

        @pl.when(exists(rel, slot))
        def _():
            stage_now = stage.at[lax.rem(step, 2)]
            stage_now[...] = product(rel, slot, 1 - core)

            @pl.when(slot == 0)
            def _():
                pack_symmetric(stage_now)

            pair_copy(step).start()
            mine[...] = product(rel, slot, core)

            @pl.when(slot == 0)
            def _():
                pack_symmetric(mine)
                pair_copy(step).wait_recv()
                finish(rel, slot, True)

            @pl.when(slot > 0)
            def _():
                pair_copy(step).wait_recv()
                finish(rel, slot, False)

            pair_copy(step).wait_send()

        return carry

    pair_copy(0, 2 * STRIP).wait_send()
    lax.fori_loop(1, STEPS, body, 0)

    def arrived(slot, m, first):
        near_send(ALONG_X, slot, m, first).wait_recv()
        near_send(ALONG_Y, slot, m, first).wait_recv()
        return (piece(acc.at[HERE, slot], m, first)[...] + piece(from_x.at[slot], m, first)[...]
                + piece(from_y.at[slot], m, first)[...])

    unpack_symmetric(out_ref.at[0, 0], arrived(0, 0, True), arrived(0, 1, True))
    for slot in range(1, SLOTS):
        @pl.when(exists(HERE, slot))
        def _(slot=slot):
            for m in pieces(False):
                out_ref[0, slot, m * STRIP:(m + 1) * STRIP] = arrived(slot, m, False)

    @pl.when(jnp.logical_not(exists(HERE, SLOTS - 1)))
    def _():
        out_ref[0, SLOTS - 1] = jnp.zeros((BLK, BLK), jnp.float32)

    for rel in (DIAG, ALONG_X, ALONG_Y):
        for slot in range(SLOTS):
            @pl.when(exists(rel, slot))
            def _(rel=rel, slot=slot):
                first = slot == 0
                for m in pieces(first):
                    if rel == DIAG:
                        far_send(slot, m, first, True).wait_send()
                    else:
                        near_send(rel, slot, m, first).wait_send()


def solution(mesh):
    def local_gram(a_local):
        block = (SLOTS, BLK, BLK)
        dma = pltpu.SemaphoreType.DMA
        return pl.pallas_call(
            gram_kernel,
            out_shape=pltpu.VMEM((1,) + block, jnp.float32),
            in_specs=[pl.BlockSpec(memory_space=pl.ANY)],
            out_specs=pl.BlockSpec(memory_space=pltpu.VMEM),
            scratch_shapes=[
                pltpu.VMEM(a_local.shape, a_local.dtype),
                pltpu.VMEM((4,) + block, jnp.float32),
                pltpu.VMEM((2, BLK, BLK), jnp.float32),
                pltpu.VMEM((BLK, BLK), jnp.float32),
                pltpu.VMEM(block, jnp.float32),
                pltpu.VMEM(block, jnp.float32),
                pltpu.VMEM(block, jnp.float32),
                pltpu.VMEM(block, jnp.float32),
                dma((GROUPS + 1,)),
                dma((2,)),
                dma((4, SLOTS)),
                dma((3, SLOTS, 3)),
                dma((SLOTS, 3)),
                dma((SLOTS, 3)),
                dma((SLOTS, 3)),
                dma((SLOTS, 3)),
            ],
            compiler_params=pltpu.CompilerParams(
                collective_id=0, has_side_effects=True, vmem_limit_bytes=56623104),
        )(a_local)

    return jax.shard_map(local_gram, mesh=mesh, in_specs=(P('mat', 'dp'),), out_specs=P(('mat', 'dp')), check_vma=False)
```

```python
import functools

import jax
import jax.numpy as jnp
from jax import lax
from jax.experimental import pallas as pl
from jax.experimental.pallas import tpu as pltpu
from jax.sharding import PartitionSpec as P

MESH = pl.DeviceIdType.MESH
BLK = 384
STRIP = 128
GROUPS = 8
SLOTS = 5
DIAG, ALONG_X, ALONG_Y, HERE = range(4)
STEPS = 20


def square(rows=STRIP):
    return (lax.broadcasted_iota(jnp.int32, (rows, STRIP), 0), lax.broadcasted_iota(jnp.int32, (rows, STRIP), 1))


FOLD = STRIP // 2
CORNER = FOLD + 8


def pack_left(block):
    row, col = square()
    s11 = block[1, STRIP:2 * STRIP]
    block[0, 0:STRIP] = jnp.where(row >= col, block[0, 0:STRIP], s11)
    block[1, 0:STRIP] = block[1, 2 * STRIP:]
    main = jnp.sum(jnp.where(row == col, s11, 0.0), axis=0, keepdims=True)
    block[2, FOLD:CORNER] = jnp.where(square(8)[0] == 0, main, 0.0)


def pack_corner(block):
    row, col = square(FOLD)
    upper = block[2, 2 * STRIP:2 * STRIP + FOLD]
    lower = block[2, 2 * STRIP + FOLD:]
    main = jnp.sum(jnp.where(row == col, upper, 0.0), axis=0, keepdims=True)
    block[2, 0:FOLD] = jnp.where(col - FOLD > row, pltpu.roll(upper, FOLD, 1), lower)
    block[2, FOLD:CORNER] = jnp.where(square(8)[0] == 1, main, block[2, FOLD:CORNER])


def unpack_symmetric(ref, left, s21, corner):
    row, col = square()
    both, s10, s20 = left[0:STRIP], left[STRIP:2 * STRIP], left[2 * STRIP:]
    both_t = both.T
    fold = corner[0:FOLD]
    low = jnp.concatenate([pltpu.roll(fold, FOLD, 1), fold], axis=0)
    straight = jnp.where(jnp.maximum(row, col) >= FOLD, row - col, col - row) >= 0
    s22 = jnp.where(straight, low, low.T)
    ref[0:STRIP, 0:STRIP] = jnp.where(row >= col, both, both_t)
    ref[STRIP:2 * STRIP, STRIP:2 * STRIP] = jnp.where(
        row == col, corner[FOLD:FOLD + 1], jnp.where(row < col, both, both_t))
    ref[2 * STRIP:, 2 * STRIP:] = jnp.where(
        jnp.logical_and(row == col, row < FOLD), corner[FOLD + 1:FOLD + 2], s22)
    ref[STRIP:2 * STRIP, 0:STRIP] = s10
    ref[0:STRIP, STRIP:2 * STRIP] = s10.T
    ref[2 * STRIP:, 0:STRIP] = s20
    ref[0:STRIP, 2 * STRIP:] = s20.T
    ref[2 * STRIP:, STRIP:2 * STRIP] = s21
    ref[STRIP:2 * STRIP, 2 * STRIP:] = s21.T


def gram_kernel(a_hbm, out_ref, a_buf, acc, stage, mine, from_x, from_y, relay_x, relay_y,
                load_sem, stage_sem, pair_sem, send_sem, fx_sem, fy_sem, rx_sem, ry_sem):
    me = lax.axis_index('dp')
    core = lax.rem(me, 2)
    x = lax.rem(me // 2, 2)
    y = me // 4
    half = a_buf.shape[1] // 2

    def device(xx, yy, kk):
        return (yy * 2 + xx) * 2 + kk

    pair = device(x, y, 1 - core)
    nbr_x = device(1 - x, y, core)
    nbr_y = device(x, 1 - y, core)

    barrier = pltpu.get_barrier_semaphore()
    for other in (pair, nbr_x, nbr_y):
        pl.semaphore_signal(barrier, inc=1, device_id={'dp': other}, device_id_type=MESH)

    far = device(1 - x, 1 - y, 0)

    def load(n, part=None):
        if isinstance(n, int) and n < 2:
            row = far + (1 - core if n == 0 else core)
        else:
            row = lax.rem(far + 1 - n + GROUPS, GROUPS)
        rows = pl.ds(pl.multiple_of(row * BLK, BLK), BLK)
        if part is None:
            return pltpu.make_async_copy(a_hbm.at[rows, :], a_buf.at[rows, :], load_sem.at[n])
        cols = pl.ds(part * half, half)
        return pltpu.make_async_copy(a_hbm.at[rows, cols], a_buf.at[rows, cols], load_sem.at[GROUPS * part])

    load(0, 0).start()
    load(0, 1).start()
    for n in range(1, GROUPS):
        load(n).start()

    near_first = ALONG_X + y
    near_second = ALONG_Y - y

    def step_task(step):
        mid = step - SLOTS
        in_mid = jnp.logical_and(mid >= 0, mid < 2 * SLOTS)
        near = jnp.where(lax.rem(mid + 2 * SLOTS, 2) == 0, near_first, near_second)
        rel = jnp.where(step < SLOTS, DIAG, jnp.where(in_mid, near, HERE))
        slot = jnp.where(step < SLOTS, step, jnp.where(in_mid, mid // 2, step - 3 * SLOTS))
        return rel, slot

    def dest_xy(rel):
        flip_x = jnp.where(rel <= ALONG_X, 1, 0)
        flip_y = jnp.where(lax.rem(rel, 2) == 0, 1, 0)
        xx = x + flip_x - 2 * flip_x * x
        yy = y + flip_y - 2 * flip_y * y
        return xx, yy

    def exists(rel, slot):
        _, yy = dest_xy(rel)
        return jnp.logical_or(slot < SLOTS - 1, yy == 0)

    def dot(lo, lo_rows, hi, hi_rows, cols=slice(None)):
        return lax.dot_general(a_buf[pl.ds(lo, lo_rows), cols], a_buf[pl.ds(hi, hi_rows), cols],
                               (((1,), (1,)), ((), ())), preferred_element_type=jnp.float32)

    def block_rows(rel, slot, kk):
        xx, yy = dest_xy(rel)
        p = device(xx, yy, kk)
        q = lax.rem(p - slot + GROUPS, GROUPS)
        hi = pl.multiple_of(jnp.maximum(p, q) * BLK, BLK)
        lo = pl.multiple_of(jnp.minimum(p, q) * BLK, BLK)
        return hi, lo

    def product(block, hi, lo, first=0, count=3):
        val = dot(hi, BLK, lo + first * STRIP, count * STRIP)
        for m in range(count):
            block[first + m] = val[:, m * STRIP:(m + 1) * STRIP]

    def part(ref, m, first):
        if first and m:
            return ref.at[m, pl.ds(0, STRIP if m == 1 else CORNER)]
        return ref.at[m]

    def pair_copy(rel, slot, src, dst, m=0):
        return pltpu.make_async_remote_copy(
            src_ref=src, dst_ref=dst, send_sem=stage_sem.at[m], recv_sem=pair_sem.at[rel, slot, m],
            device_id={'dp': pair}, device_id_type=MESH)

    def pair_block(rel, slot):
        return pair_copy(rel, slot, stage.at[0], acc.at[rel, slot])

    def by_y(ordinal, dest_x, dest_y):
        later = ordinal - 3
        n, o = 5 - core, 7 + core
        short = (later * 2 + 3) // 3 - (later * 2 + 1) // 3
        full = ((later + 1) * n + o) // 12 - (later * n + o) // 12
        small = jnp.where(jnp.logical_and(dest_x == 1, dest_y == 0), 0, 1 - core)
        early = jnp.where(ordinal == 0, core, small)
        return jnp.where(ordinal < 3, early, jnp.where(dest_y == 1, short, full)) == 1

    def ordinal(slot, m, first):
        return m if first else 3 * slot + m

    def far_send(slot, m, first, along_y):
        return pltpu.make_async_remote_copy(
            src_ref=part(acc.at[DIAG, slot], m, first),
            dst_ref=part((relay_x if along_y else relay_y).at[slot], m, first),
            send_sem=send_sem.at[DIAG, slot, m],
            recv_sem=(rx_sem if along_y else ry_sem).at[slot, m],
            device_id={'dp': nbr_y if along_y else nbr_x}, device_id_type=MESH)

    def near_send(rel, slot, m, first):
        along_y = rel == ALONG_Y
        return pltpu.make_async_remote_copy(
            src_ref=part(acc.at[rel, slot], m, first),
            dst_ref=part((from_y if along_y else from_x).at[slot], m, first),
            send_sem=send_sem.at[rel, slot, m],
            recv_sem=(fy_sem if along_y else fx_sem).at[slot, m],
            device_id={'dp': nbr_y if along_y else nbr_x}, device_id_type=MESH)

    def finish(rel, slot, m, first, only_far=False):
        total = part(acc.at[rel, slot], m, first)
        total[...] = total[...] + part(mine, m, first)[...]

        def send_far():
            along_y = by_y(ordinal(slot, m, first), 1 - x, 1 - y)

            @pl.when(along_y)
            def _():
                far_send(slot, m, first, True).start()

            @pl.when(jnp.logical_not(along_y))
            def _():
                far_send(slot, m, first, False).start()

        if only_far:
            send_far()
            return
        pl.when(rel == DIAG)(send_far)

        @pl.when(rel == ALONG_X)
        def _():
            @pl.when(by_y(ordinal(slot, m, first), 1 - x, y))
            def _():
                far_send(slot, m, first, True).wait_recv()
                total = part(acc.at[ALONG_X, slot], m, first)
                total[...] = total[...] + part(relay_x.at[slot], m, first)[...]

            near_send(ALONG_X, slot, m, first).start()

        @pl.when(rel == ALONG_Y)
        def _():
            @pl.when(jnp.logical_not(by_y(ordinal(slot, m, first), x, 1 - y)))
            def _():
                far_send(slot, m, first, False).wait_recv()
                total = part(acc.at[ALONG_Y, slot], m, first)
                total[...] = total[...] + part(relay_y.at[slot], m, first)[...]

            near_send(ALONG_Y, slot, m, first).start()

    def start_part(slot, m, first):
        copy = pair_copy(DIAG, slot, part(stage.at[slot], m, first), part(acc.at[DIAG, slot], m, first), 3 * slot + m)
        return copy

    def left_product(block, kk, halves):
        row = pl.multiple_of((far + kk) * BLK, BLK)
        for h in range(halves):
            if halves > 1:
                load(0, h).wait()
            cols = pl.ds(h * half, half) if halves > 1 else slice(None)
            val = dot(row, BLK, row, 2 * STRIP, cols)
            for m in range(2):
                now = val[:, m * STRIP:(m + 1) * STRIP]
                block[m] = block[m] + now if h else now
        pack_left(block)

    def corner_product(block, kk):
        row = pl.multiple_of((far + kk) * BLK + 2 * STRIP, STRIP)
        block[2, 2 * STRIP:] = dot(row, STRIP, row, STRIP)
        pack_corner(block)

    def start_finish(slot, parts, first):
        for m in parts:
            start_part(slot, m, first).wait_recv()
            finish(DIAG, slot, m, first, only_far=True)

    left_product(stage.at[0], 1 - core, 2)
    pl.semaphore_wait(barrier, 3)
    start_part(0, 0, True).start()
    start_part(0, 1, True).start()
    load(1).wait()
    left_product(mine, core, 1)
    corner_product(stage.at[0], 1 - core)
    start_part(0, 2, True).start()
    start_finish(0, (0, 1), True)
    corner_product(mine, core)
    load(2).wait()
    product(stage.at[1], *block_rows(DIAG, 1, 1 - core), 0, 2)
    start_part(1, 0, False).start()
    start_part(1, 1, False).start()
    start_finish(0, (2,), True)
    product(mine, *block_rows(DIAG, 1, core), 0, 2)
    product(stage.at[1], *block_rows(DIAG, 1, 1 - core), 2, 1)
    start_part(1, 2, False).start()
    start_finish(1, (0, 1), False)
    product(mine, *block_rows(DIAG, 1, core), 2, 1)
    start_finish(1, (2,), False)
    for m in range(3):
        start_part(0, m, True).wait_send()
        start_part(1, m, False).wait_send()

    def body(step, carry):
        @pl.when(step < SLOTS + 1)
        def _():
            load(step + 1).wait()

        @pl.when(step == SLOTS)
        def _():
            load(GROUPS - 1).wait()

        rel, slot = step_task(step)

        @pl.when(exists(rel, slot))
        def _():
            product(stage.at[0], *block_rows(rel, slot, 1 - core))

            @pl.when(slot == 0)
            def _():
                pack_left(stage.at[0])
                pack_corner(stage.at[0])

            pair_block(rel, slot).start()
            product(mine, *block_rows(rel, slot, core))

            @pl.when(slot == 0)
            def _():
                pack_left(mine)
                pack_corner(mine)
                pair_block(rel, slot).wait_recv()
                for m in range(3):
                    finish(rel, slot, m, True)

            @pl.when(slot > 0)
            def _():
                pair_block(rel, slot).wait_recv()
                for m in range(3):
                    finish(rel, slot, m, False)

            pair_block(rel, slot).wait_send()

        return carry

    lax.fori_loop(2, STEPS, body, 0)

    def arrived(slot, m, first):
        near_send(ALONG_X, slot, m, first).wait_recv()
        near_send(ALONG_Y, slot, m, first).wait_recv()
        return (part(acc.at[HERE, slot], m, first)[...] + part(from_x.at[slot], m, first)[...]
                + part(from_y.at[slot], m, first)[...])

    unpack_symmetric(out_ref.at[0, 0], *(arrived(0, m, True) for m in range(3)))
    for slot in range(1, SLOTS):
        @pl.when(exists(HERE, slot))
        def _(slot=slot):
            for m in range(3):
                out_ref[0, slot, :, m * STRIP:(m + 1) * STRIP] = arrived(slot, m, False)

    @pl.when(jnp.logical_not(exists(HERE, SLOTS - 1)))
    def _():
        out_ref[0, SLOTS - 1] = jnp.zeros((BLK, BLK), jnp.float32)

    for rel in (DIAG, ALONG_X, ALONG_Y):
        for slot in range(SLOTS):
            @pl.when(exists(rel, slot))
            def _(rel=rel, slot=slot):
                for m in range(3):
                    if rel == DIAG:
                        far_send(slot, m, slot == 0, True).wait_send()
                    else:
                        near_send(rel, slot, m, slot == 0).wait_send()


def solution(mesh):
    def local_gram(a_local):
        held = (SLOTS, 3, BLK, STRIP)
        dma = pltpu.SemaphoreType.DMA
        return pl.pallas_call(
            gram_kernel,
            out_shape=pltpu.VMEM((1, SLOTS, BLK, BLK), jnp.float32),
            in_specs=[pl.BlockSpec(memory_space=pl.ANY)],
            out_specs=pl.BlockSpec(memory_space=pltpu.VMEM),
            scratch_shapes=[
                pltpu.VMEM(a_local.shape, a_local.dtype),
                pltpu.VMEM((4,) + held, jnp.float32),
                pltpu.VMEM((2,) + held[1:], jnp.float32),
                pltpu.VMEM(held[1:], jnp.float32),
                pltpu.VMEM(held, jnp.float32),
                pltpu.VMEM(held, jnp.float32),
                pltpu.VMEM(held, jnp.float32),
                pltpu.VMEM(held, jnp.float32),
                dma((GROUPS + 1,)),
                dma((6,)),
                dma((4, SLOTS, 6)),
                dma((3, SLOTS, 3)),
                dma((SLOTS, 3)),
                dma((SLOTS, 3)),
                dma((SLOTS, 3)),
                dma((SLOTS, 3)),
            ],
            compiler_params=pltpu.CompilerParams(
                collective_id=0, has_side_effects=True, vmem_limit_bytes=56623104),
        )(a_local)

    return jax.shard_map(local_gram, mesh=mesh, in_specs=(P('mat', 'dp'),), out_specs=P(('mat', 'dp')), check_vma=False)
```

```python
import functools

import jax
import jax.numpy as jnp
from jax import lax
from jax.experimental import pallas as pl
from jax.experimental.pallas import tpu as pltpu
from jax.sharding import PartitionSpec as P

MESH = pl.DeviceIdType.MESH
BLK = 384
STRIP = 128
ROWS = 3 * BLK
GROUPS = 8
SLOTS = 5
DIAG, ALONG_X, ALONG_Y, HERE = range(4)
STEPS = 20


def square(rows=STRIP):
    return (lax.broadcasted_iota(jnp.int32, (rows, STRIP), 0), lax.broadcasted_iota(jnp.int32, (rows, STRIP), 1))


FOLD = STRIP // 2
CORNER = FOLD + 8
FIRST_PARTS = (BLK, STRIP, CORNER)


def rows_of(m, start, stop):
    return slice(m * BLK + start, m * BLK + stop)


def pack_left(block):
    row, col = square()
    s11 = block[rows_of(1, STRIP, 2 * STRIP)]
    block[rows_of(0, 0, STRIP)] = jnp.where(row >= col, block[rows_of(0, 0, STRIP)], s11)
    block[rows_of(1, 0, STRIP)] = block[rows_of(1, 2 * STRIP, BLK)]
    main = jnp.sum(jnp.where(row == col, s11, 0.0), axis=0, keepdims=True)
    block[rows_of(2, FOLD, CORNER)] = jnp.where(square(8)[0] == 0, main, 0.0)


def pack_corner(block):
    row, col = square(FOLD)
    upper = block[rows_of(2, 2 * STRIP, 2 * STRIP + FOLD)]
    lower = block[rows_of(2, 2 * STRIP + FOLD, BLK)]
    main = jnp.sum(jnp.where(row == col, upper, 0.0), axis=0, keepdims=True)
    block[rows_of(2, 0, FOLD)] = jnp.where(col - FOLD > row, pltpu.roll(upper, FOLD, 1), lower)
    block[rows_of(2, FOLD, CORNER)] = jnp.where(square(8)[0] == 1, main, block[rows_of(2, FOLD, CORNER)])


def unpack_symmetric(ref, left, s21, corner):
    row, col = square()
    both, s10, s20 = left[0:STRIP], left[STRIP:2 * STRIP], left[2 * STRIP:]
    both_t = both.T
    fold = corner[0:FOLD]
    low = jnp.concatenate([pltpu.roll(fold, FOLD, 1), fold], axis=0)
    straight = jnp.where(jnp.maximum(row, col) >= FOLD, row - col, col - row) >= 0
    s22 = jnp.where(straight, low, low.T)
    ref[0:STRIP, 0:STRIP] = jnp.where(row >= col, both, both_t)
    ref[STRIP:2 * STRIP, STRIP:2 * STRIP] = jnp.where(
        row == col, corner[FOLD:FOLD + 1], jnp.where(row < col, both, both_t))
    ref[2 * STRIP:, 2 * STRIP:] = jnp.where(
        jnp.logical_and(row == col, row < FOLD), corner[FOLD + 1:FOLD + 2], s22)
    ref[STRIP:2 * STRIP, 0:STRIP] = s10
    ref[0:STRIP, STRIP:2 * STRIP] = s10.T
    ref[2 * STRIP:, 0:STRIP] = s20
    ref[0:STRIP, 2 * STRIP:] = s20.T
    ref[2 * STRIP:, STRIP:2 * STRIP] = s21
    ref[STRIP:2 * STRIP, 2 * STRIP:] = s21.T


def part(block, m, first):
    return block.at[pl.ds(m * BLK, FIRST_PARTS[m] if first else BLK)]


def gram_kernel(a_hbm, out_ref, a_buf, acc, stage, stage_next, mine, from_x, from_y, relay_x, relay_y,
                load_sem, stage_sem, pair_sem, send_sem, fx_sem, fy_sem, rx_sem, ry_sem):
    me = lax.axis_index('dp')
    core = lax.rem(me, 2)
    x = lax.rem(me // 2, 2)
    y = me // 4
    half = a_buf.shape[1] // 2
    one = 1 + me // GROUPS

    def device(xx, yy, kk):
        return (yy * 2 + xx) * 2 + kk

    pair = device(x, y, 1 - core)
    nbr_x = device(1 - x, y, core)
    nbr_y = device(x, 1 - y, core)

    barrier = pltpu.get_barrier_semaphore()
    for other in (pair, nbr_x, nbr_y):
        pl.semaphore_signal(barrier, inc=1, device_id={'dp': other}, device_id_type=MESH)

    far = device(1 - x, 1 - y, 0)

    def load(n):
        row = far + core if isinstance(n, int) and n == 1 else lax.rem(far + 1 - n + GROUPS, GROUPS)
        rows = pl.ds(pl.multiple_of(row * BLK, BLK), BLK)
        return pltpu.make_async_copy(a_hbm.at[rows, :], a_buf.at[rows, :], load_sem.at[n])

    def load_half(h):
        rows = pl.ds(pl.multiple_of((far + 1 - core) * BLK, BLK), BLK)
        cols = pl.ds(pl.multiple_of(h * half, half), half)
        return pltpu.make_async_copy(a_hbm.at[rows, cols], a_buf.at[rows, cols], load_sem.at[GROUPS * h])

    load_half(0).start()
    load_half(1).start()
    for n in range(1, GROUPS):
        load(n).start()

    near_first = ALONG_X + y
    near_second = ALONG_Y - y

    def step_task(step):
        mid = step - SLOTS
        in_mid = jnp.logical_and(mid >= 0, mid < 2 * SLOTS)
        near = jnp.where(lax.rem(mid + 2 * SLOTS, 2) == 0, near_first, near_second)
        rel = jnp.where(step < SLOTS, DIAG, jnp.where(in_mid, near, HERE))
        slot = jnp.where(step < SLOTS, step, jnp.where(in_mid, mid // 2, step - 3 * SLOTS))
        return rel, slot

    def dest_xy(rel):
        flip_x = jnp.where(rel <= ALONG_X, 1, 0)
        flip_y = jnp.where(lax.rem(rel, 2) == 0, 1, 0)
        xx = x + flip_x - 2 * flip_x * x
        yy = y + flip_y - 2 * flip_y * y
        return xx, yy

    def exists(rel, slot):
        _, yy = dest_xy(rel)
        return jnp.logical_or(slot < SLOTS - 1, yy == 0)

    def held(ref, slot):
        return ref.at[pl.ds(pl.multiple_of(slot * ROWS, ROWS), ROWS)]

    def total_of(rel, slot):
        return held(acc, rel * SLOTS + slot)

    def dot(left, left_rows, right, right_rows, cols=slice(None)):
        return lax.dot_general(a_buf[pl.ds(left, left_rows), cols], a_buf[pl.ds(right, right_rows), cols],
                               (((1,), (1,)), ((), ())), preferred_element_type=jnp.float32)

    def block_rows(rel, slot, kk):
        xx, yy = dest_xy(rel)
        p = device(xx, yy, kk)
        q = lax.rem(p - slot + GROUPS, GROUPS)
        hi = pl.multiple_of(jnp.maximum(p, q) * BLK, BLK)
        lo = pl.multiple_of(jnp.minimum(p, q) * BLK, BLK)
        return hi, lo

    def product(block, hi, lo, first=0, count=3):
        val = dot(hi, BLK, lo + first * STRIP, count * STRIP)
        for m in range(count):
            block[rows_of(first + m, 0, BLK)] = val[:, m * STRIP:(m + 1) * STRIP]

    def alone(work):
        def run(_, carry):
            work()
            return carry

        lax.fori_loop(0, one, run, 0)

    def pair_copy(src, dst, send, recv):
        return pltpu.make_async_remote_copy(
            src_ref=src, dst_ref=dst, send_sem=stage_sem.at[send], recv_sem=pair_sem.at[recv],
            device_id={'dp': pair}, device_id_type=MESH)

    def pair_block(step):
        return pair_copy(stage, total_of(*step_task(step)), 0, 5 + lax.rem(step, 3))

    def by_y(ordinal, dest_x, dest_y):
        later = ordinal - 3
        n = jnp.where(dest_x == 1, 4 + core, 5 - core)
        short = (later * 2 + 3) // 3 - (later * 2 + 1) // 3
        full = (later * n + 12) // 12 - (later * n + 12 - n) // 12
        early = jnp.where(ordinal == 0, core, 1 - core)
        return jnp.where(ordinal < 3, early, jnp.where(dest_y == 1, short, full)) == 1

    def ordinal(slot, m, first):
        return m if first else 3 * slot + m

    def far_send(slot, m, first, along_y):
        return pltpu.make_async_remote_copy(
            src_ref=part(total_of(DIAG, slot), m, first),
            dst_ref=part(held(relay_x if along_y else relay_y, slot), m, first),
            send_sem=send_sem.at[DIAG],
            recv_sem=(rx_sem if along_y else ry_sem).at[slot, m],
            device_id={'dp': nbr_y if along_y else nbr_x}, device_id_type=MESH)

    def near_send(rel, slot, m, first):
        along_y = rel == ALONG_Y
        return pltpu.make_async_remote_copy(
            src_ref=part(total_of(rel, slot), m, first),
            dst_ref=part(held(from_y if along_y else from_x, slot), m, first),
            send_sem=send_sem.at[rel],
            recv_sem=(fy_sem if along_y else fx_sem).at[slot],
            device_id={'dp': nbr_y if along_y else nbr_x}, device_id_type=MESH)

    def finish(rel, slot, m, first, only_far=False):
        total = part(total_of(rel, slot), m, first)
        total[...] = total[...] + part(mine, m, first)[...]

        def send_far():
            along_y = by_y(ordinal(slot, m, first), 1 - x, 1 - y)

            @pl.when(along_y)
            def _():
                far_send(slot, m, first, True).start()

            @pl.when(jnp.logical_not(along_y))
            def _():
                far_send(slot, m, first, False).start()

        if only_far:
            send_far()
            return
        pl.when(rel == DIAG)(send_far)

        @pl.when(rel == ALONG_X)
        def _():
            @pl.when(by_y(ordinal(slot, m, first), 1 - x, y))
            def _():
                far_send(slot, m, first, True).wait_recv()
                total = part(total_of(ALONG_X, slot), m, first)
                total[...] = total[...] + part(held(relay_x, slot), m, first)[...]

            near_send(ALONG_X, slot, m, first).start()

        @pl.when(rel == ALONG_Y)
        def _():
            @pl.when(jnp.logical_not(by_y(ordinal(slot, m, first), x, 1 - y)))
            def _():
                far_send(slot, m, first, False).wait_recv()
                total = part(total_of(ALONG_Y, slot), m, first)
                total[...] = total[...] + part(held(relay_y, slot), m, first)[...]

            near_send(ALONG_Y, slot, m, first).start()

    def left_half(block, kk, h):
        row = pl.multiple_of((far + kk) * BLK, BLK)
        val = dot(row, BLK, row, 2 * STRIP, pl.ds(pl.multiple_of(h * half, half), half))
        for m in range(2):
            block[rows_of(m, 0, BLK)] = (
                jnp.where(h > 0, block[rows_of(m, 0, BLK)], 0.0) + val[:, m * STRIP:(m + 1) * STRIP])

    def left_product(block, kk):
        row = pl.multiple_of((far + kk) * BLK, BLK)
        val = dot(row, BLK, row, 2 * STRIP)
        for m in range(2):
            block[rows_of(m, 0, BLK)] = val[:, m * STRIP:(m + 1) * STRIP]

    def corner_product(block, kk):
        row = pl.multiple_of((far + kk) * BLK + 2 * STRIP, STRIP)
        block[rows_of(2, 2 * STRIP, BLK)] = dot(row, STRIP, row, STRIP)

    def first_half(h, carry):
        load_half(h).wait()
        left_half(stage, 1 - core, h)
        return carry

    two = pl.ds(0, 2 * BLK)
    first_total, next_total = total_of(DIAG, 0), total_of(DIAG, 1)
    copies = (
        pair_copy(part(stage, 0, True), part(first_total, 0, True), 0, 0),
        pair_copy(part(stage, 1, True), part(first_total, 1, True), 1, 1),
        pair_copy(part(stage, 2, True), part(first_total, 2, True), 2, 2),
        pair_copy(stage_next.at[two], next_total.at[two], 3, 3),
        pair_copy(part(stage_next, 2, False), part(next_total, 2, False), 4, 4),
    )

    lax.fori_loop(0, 2 * one, first_half, 0)
    pack_left(stage)
    pl.semaphore_wait(barrier, 3)
    copies[0].start()
    copies[1].start()
    load(1).wait()
    alone(lambda: left_product(mine, core))
    pack_left(mine)
    alone(lambda: corner_product(stage, 1 - core))
    pack_corner(stage)
    copies[2].start()
    copies[0].wait_recv()
    finish(DIAG, 0, 0, True, only_far=True)
    copies[1].wait_recv()
    finish(DIAG, 0, 1, True, only_far=True)
    load(2).wait()
    alone(lambda: product(stage_next, *block_rows(DIAG, 1, 1 - core), 0, 2))
    copies[3].start()
    alone(lambda: corner_product(mine, core))
    pack_corner(mine)
    copies[2].wait_recv()
    finish(DIAG, 0, 2, True, only_far=True)
    alone(lambda: product(mine, *block_rows(DIAG, 1, core), 0, 2))
    copies[3].wait_recv()
    finish(DIAG, 1, 0, False, only_far=True)
    finish(DIAG, 1, 1, False, only_far=True)
    alone(lambda: product(stage_next, *block_rows(DIAG, 1, 1 - core), 2, 1))
    copies[4].start()
    alone(lambda: product(mine, *block_rows(DIAG, 1, core), 2, 1))
    copies[4].wait_recv()
    finish(DIAG, 1, 2, False, only_far=True)
    for copy in copies:
        copy.wait_send()

    def body(step, carry):
        @pl.when(step < SLOTS + 1)
        def _():
            load(step + 1).wait()

        @pl.when(step == SLOTS)
        def _():
            load(GROUPS - 1).wait()

        rel, slot = step_task(step)

        @pl.when(exists(rel, slot))
        def _():
            product(stage, *block_rows(rel, slot, 1 - core))

            @pl.when(slot == 0)
            def _():
                pack_left(stage)
                pack_corner(stage)

            pair_block(step).start()
            product(mine, *block_rows(rel, slot, core))

            @pl.when(slot == 0)
            def _():
                pack_left(mine)
                pack_corner(mine)
                pair_block(step).wait_recv()
                for m in range(3):
                    finish(rel, slot, m, True)

            @pl.when(slot > 0)
            def _():
                pair_block(step).wait_recv()
                for m in range(3):
                    finish(rel, slot, m, False)

            pair_block(step).wait_send()

        return carry

    lax.fori_loop(2, STEPS, body, 0)

    def arrived(slot):
        first = slot == 0
        size = pl.ds(0, sum(FIRST_PARTS) if first else ROWS)
        for ref, sem in ((from_x, fx_sem), (from_y, fy_sem)):
            whole = held(ref, slot).at[size]
            pltpu.make_async_copy(whole, whole, sem.at[slot]).wait()
        for m in range(3):
            yield (part(total_of(HERE, slot), m, first)[...] + part(held(from_x, slot), m, first)[...]
                   + part(held(from_y, slot), m, first)[...])

    unpack_symmetric(out_ref.at[0, 0], *arrived(0))
    for slot in range(1, SLOTS):
        @pl.when(exists(HERE, slot))
        def _(slot=slot):
            for m, total in enumerate(arrived(slot)):
                out_ref[0, slot, :, m * STRIP:(m + 1) * STRIP] = total

    @pl.when(jnp.logical_not(exists(HERE, SLOTS - 1)))
    def _():
        out_ref[0, SLOTS - 1] = jnp.zeros((BLK, BLK), jnp.float32)

    for rel in (DIAG, ALONG_X, ALONG_Y):
        for slots in (SLOTS - 1, SLOTS):
            @pl.when(exists(rel, SLOTS - 1) == (slots == SLOTS))
            def _(rel=rel, slots=slots):
                everything = acc.at[pl.ds(0, sum(FIRST_PARTS) + (slots - 1) * ROWS)]
                pltpu.make_async_copy(everything, everything, send_sem.at[rel]).wait()


def solution(mesh):
    def local_gram(a_local):
        dma = pltpu.SemaphoreType.DMA

        def blocks(n):
            return pltpu.VMEM((n * ROWS, STRIP), jnp.float32)

        return pl.pallas_call(
            gram_kernel,
            out_shape=pltpu.VMEM((1, SLOTS, BLK, BLK), jnp.float32),
            in_specs=[pl.BlockSpec(memory_space=pl.ANY)],
            out_specs=pl.BlockSpec(memory_space=pltpu.VMEM),
            scratch_shapes=[
                pltpu.VMEM(a_local.shape, a_local.dtype),
                blocks(4 * SLOTS), blocks(1), blocks(1), blocks(1),
                blocks(SLOTS), blocks(SLOTS), blocks(SLOTS), blocks(SLOTS),
                dma((GROUPS + 1,)), dma((5,)), dma((8,)), dma((3,)),
                dma((SLOTS,)), dma((SLOTS,)), dma((SLOTS, 3)), dma((SLOTS, 3)),
            ],
            compiler_params=pltpu.CompilerParams(
                collective_id=0, has_side_effects=True, vmem_limit_bytes=56623104),
        )(a_local)

    return jax.shard_map(local_gram, mesh=mesh, in_specs=(P('mat', 'dp'),), out_specs=P(('mat', 'dp')), check_vma=False)
```

```python
import functools

import jax
import jax.numpy as jnp
from jax import lax
from jax.experimental import pallas as pl
from jax.experimental.pallas import tpu as pltpu
from jax.sharding import PartitionSpec as P

MESH = pl.DeviceIdType.MESH
BLK = 384
STRIP = 128
ROWS = 3 * BLK
GROUPS = 8
SLOTS = 5
DIAG, ALONG_X, ALONG_Y, HERE = range(4)
STEPS = 4 * SLOTS - 1


def square(rows=STRIP):
    return (lax.broadcasted_iota(jnp.int32, (rows, STRIP), 0), lax.broadcasted_iota(jnp.int32, (rows, STRIP), 1))


FOLD = STRIP // 2
CORNER = FOLD + 8
FIRST_PARTS = ((0, BLK), (BLK, STRIP), (2 * BLK, CORNER))
HALF_PIECE = BLK // 2
PARTS = ((0, BLK), (BLK, BLK), (2 * BLK, HALF_PIECE), (2 * BLK + HALF_PIECE, HALF_PIECE))


def rows_of(m, start, stop):
    return slice(m * BLK + start, m * BLK + stop)


def pack_left(block):
    row, col = square()
    s11 = block[rows_of(1, STRIP, 2 * STRIP)]
    block[rows_of(0, 0, STRIP)] = jnp.where(row >= col, block[rows_of(0, 0, STRIP)], s11)
    block[rows_of(1, 0, STRIP)] = block[rows_of(1, 2 * STRIP, BLK)]
    main = jnp.sum(jnp.where(row == col, s11, 0.0), axis=0, keepdims=True)
    block[rows_of(2, FOLD, CORNER)] = jnp.where(square(8)[0] == 0, main, 0.0)


def pack_corner(block):
    row, col = square(FOLD)
    upper = block[rows_of(2, 2 * STRIP, 2 * STRIP + FOLD)]
    lower = block[rows_of(2, 2 * STRIP + FOLD, BLK)]
    main = jnp.sum(jnp.where(row == col, upper, 0.0), axis=0, keepdims=True)
    block[rows_of(2, 0, FOLD)] = jnp.where(col - FOLD > row, pltpu.roll(upper, FOLD, 1), lower)
    block[rows_of(2, FOLD, CORNER)] = jnp.where(square(8)[0] == 1, main, block[rows_of(2, FOLD, CORNER)])


def unpack_symmetric(ref, left, s21, corner):
    row, col = square()
    both, s10, s20 = left[0:STRIP], left[STRIP:2 * STRIP], left[2 * STRIP:]
    both_t = both.T
    fold = corner[0:FOLD]
    low = jnp.concatenate([pltpu.roll(fold, FOLD, 1), fold], axis=0)
    straight = jnp.where(jnp.maximum(row, col) >= FOLD, row - col, col - row) >= 0
    s22 = jnp.where(straight, low, low.T)
    ref[0:STRIP, 0:STRIP] = jnp.where(row >= col, both, both_t)
    ref[STRIP:2 * STRIP, STRIP:2 * STRIP] = jnp.where(
        row == col, corner[FOLD:FOLD + 1], jnp.where(row < col, both, both_t))
    ref[2 * STRIP:, 2 * STRIP:] = jnp.where(
        jnp.logical_and(row == col, row < FOLD), corner[FOLD + 1:FOLD + 2], s22)
    ref[STRIP:2 * STRIP, 0:STRIP] = s10
    ref[0:STRIP, STRIP:2 * STRIP] = s10.T
    ref[2 * STRIP:, 0:STRIP] = s20
    ref[0:STRIP, 2 * STRIP:] = s20.T
    ref[2 * STRIP:, STRIP:2 * STRIP] = s21
    ref[STRIP:2 * STRIP, 2 * STRIP:] = s21.T


def part(block, m, first):
    return block.at[pl.ds(*(FIRST_PARTS if first else PARTS)[m])]


def parts(first):
    return range(len(FIRST_PARTS if first else PARTS))


def size(first):
    return sum(rows for _, rows in FIRST_PARTS) if first else ROWS


def gram_kernel(a_hbm, out_ref, a_buf, acc, stage, stage_next, mine, from_x, from_y, relay_x, relay_y,
                load_sem, stage_sem, pair_sem, send_sem, fx_sem, fy_sem, rx_sem, ry_sem):
    me = lax.axis_index('dp')
    core = lax.rem(me, 2)
    x = lax.rem(me // 2, 2)
    y = me // 4
    half = a_buf.shape[1] // 2
    one = 1 + me // GROUPS

    def device(xx, yy, kk):
        return (yy * 2 + xx) * 2 + kk

    pair = device(x, y, 1 - core)
    nbr_x = device(1 - x, y, core)
    nbr_y = device(x, 1 - y, core)

    barrier = pltpu.get_barrier_semaphore()
    for other in (pair, nbr_x, nbr_y):
        pl.semaphore_signal(barrier, inc=1, device_id={'dp': other}, device_id_type=MESH)

    far = device(1 - x, 1 - y, 0)

    def load(n):
        row = far + core if isinstance(n, int) and n == 1 else lax.rem(far + 1 - n + GROUPS, GROUPS)
        rows = pl.ds(pl.multiple_of(row * BLK, BLK), BLK)
        return pltpu.make_async_copy(a_hbm.at[rows, :], a_buf.at[rows, :], load_sem.at[n])

    def load_half(h):
        rows = pl.ds(pl.multiple_of((far + 1 - core) * BLK, BLK), BLK)
        cols = pl.ds(pl.multiple_of(h * half, half), half)
        return pltpu.make_async_copy(a_hbm.at[rows, cols], a_buf.at[rows, cols], load_sem.at[GROUPS * h])

    load_half(0).start()
    load_half(1).start()
    for n in range(1, GROUPS):
        load(n).start()

    near_first = ALONG_X + y
    near_second = ALONG_Y - y

    def step_task(step):
        mid = step - SLOTS
        in_mid = jnp.logical_and(mid >= 0, mid < 2 * SLOTS - 1)
        to_first = jnp.logical_or(mid <= 0, lax.rem(mid + 2 * SLOTS, 2) == 1)
        near = jnp.where(to_first, near_first, near_second)
        near_slot = jnp.where(to_first, (mid + 1) // 2, mid // 2 - 1)
        rel = jnp.where(step < SLOTS, DIAG, jnp.where(in_mid, near, HERE))
        slot = jnp.where(step < SLOTS, step, jnp.where(in_mid, near_slot, step - 3 * SLOTS + 1))
        return rel, slot

    def dest_xy(rel):
        flip_x = jnp.where(rel <= ALONG_X, 1, 0)
        flip_y = jnp.where(lax.rem(rel, 2) == 0, 1, 0)
        xx = x + flip_x - 2 * flip_x * x
        yy = y + flip_y - 2 * flip_y * y
        return xx, yy

    def exists(rel, slot):
        _, yy = dest_xy(rel)
        return jnp.logical_or(slot < SLOTS - 1, yy == 0)

    def held(ref, slot):
        return ref.at[pl.ds(pl.multiple_of(slot * ROWS, ROWS), ROWS)]

    def total_of(rel, slot):
        return held(acc, rel * SLOTS + slot)

    def dot(left, left_rows, right, right_rows, cols=slice(None)):
        return lax.dot_general(a_buf[pl.ds(left, left_rows), cols], a_buf[pl.ds(right, right_rows), cols],
                               (((1,), (1,)), ((), ())), preferred_element_type=jnp.float32)

    def block_rows(rel, slot, kk):
        xx, yy = dest_xy(rel)
        p = device(xx, yy, kk)
        q = lax.rem(p - slot + GROUPS, GROUPS)
        hi = pl.multiple_of(jnp.maximum(p, q) * BLK, BLK)
        lo = pl.multiple_of(jnp.minimum(p, q) * BLK, BLK)
        return hi, lo

    def product(block, hi, lo, first=0, count=3):
        val = dot(hi, BLK, lo + first * STRIP, count * STRIP)
        for m in range(count):
            block[rows_of(first + m, 0, BLK)] = val[:, m * STRIP:(m + 1) * STRIP]

    def alone(work):
        def run(_, carry):
            work()
            return carry

        lax.fori_loop(0, one, run, 0)

    def pair_copy(src, dst, send, recv):
        return pltpu.make_async_remote_copy(
            src_ref=src, dst_ref=dst, send_sem=stage_sem.at[send], recv_sem=pair_sem.at[recv],
            device_id={'dp': pair}, device_id_type=MESH)

    def pair_block(step):
        return pair_copy(stage, total_of(*step_task(step)), 0, 5 + lax.rem(step, 3))

    def by_y(slot, m, first, dest_x, dest_y):
        if first:
            return (core if m == 0 else 1 - core) == 1

        def listed(*bits):
            return jnp.where(slot == 1, bits[0], jnp.where(slot == 2, bits[1], jnp.where(slot == 3, bits[2], bits[3])))

        to_zero = jnp.where(core == 0, listed(13, 2, 1, 1), listed(1, 1, 2, 2))
        to_one = jnp.where(core == 0, listed(5, 2, 1, 1), listed(5, 1, 2, 4))
        bits = jnp.where(dest_y == 1, 13, jnp.where(dest_x == 0, to_zero, to_one))
        return lax.rem(bits // 2 ** m, 2) == 1

    def relay_wait(slot, first, relay, sem, flags):
        rows = sum(jnp.where(flag, part_rows, 0)
                   for flag, (_, part_rows) in zip(flags, FIRST_PARTS if first else PARTS))
        possible = (BLK, size(True) - BLK) if first else range(HALF_PIECE, ROWS + 1, HALF_PIECE)
        for count in possible:
            @pl.when(rows == count)
            def _(count=count):
                whole = held(relay, slot).at[pl.ds(0, count)]
                pltpu.make_async_copy(whole, whole, sem.at[slot]).wait()

    def far_send(slot, m, first, along_y):
        return pltpu.make_async_remote_copy(
            src_ref=part(total_of(DIAG, slot), m, first),
            dst_ref=part(held(relay_x if along_y else relay_y, slot), m, first),
            send_sem=send_sem.at[DIAG],
            recv_sem=(rx_sem if along_y else ry_sem).at[slot],
            device_id={'dp': nbr_y if along_y else nbr_x}, device_id_type=MESH)

    def near_send(rel, slot, m, first):
        along_y = rel == ALONG_Y
        return pltpu.make_async_remote_copy(
            src_ref=part(total_of(rel, slot), m, first),
            dst_ref=part(held(from_y if along_y else from_x, slot), m, first),
            send_sem=send_sem.at[rel],
            recv_sem=(fy_sem if along_y else fx_sem).at[slot],
            device_id={'dp': nbr_y if along_y else nbr_x}, device_id_type=MESH)

    def finish_far(slot, m, first):
        total = part(total_of(DIAG, slot), m, first)
        total[...] = total[...] + part(mine, m, first)[...]
        along_y = by_y(slot, m, first, 1 - x, 1 - y)

        @pl.when(along_y)
        def _():
            far_send(slot, m, first, True).start()

        @pl.when(jnp.logical_not(along_y))
        def _():
            far_send(slot, m, first, False).start()

    def finish_near(rel, slot, first):
        if rel == ALONG_X:
            relay, sem = relay_x, rx_sem
            flags = [by_y(slot, m, first, 1 - x, y) for m in parts(first)]
        else:
            relay, sem = relay_y, ry_sem
            flags = [jnp.logical_not(by_y(slot, m, first, x, 1 - y)) for m in parts(first)]
        relay_wait(slot, first, relay, sem, flags)
        for m in parts(first):
            total = part(total_of(rel, slot), m, first)

            @pl.when(flags[m])
            def _(m=m, total=total):
                total[...] = total[...] + part(mine, m, first)[...] + part(held(relay, slot), m, first)[...]

            @pl.when(jnp.logical_not(flags[m]))
            def _(m=m, total=total):
                total[...] = total[...] + part(mine, m, first)[...]

            near_send(rel, slot, m, first).start()

    def finish(rel, slot, first):
        @pl.when(rel == DIAG)
        def _():
            for m in parts(first):
                finish_far(slot, m, first)

        for near in (ALONG_X, ALONG_Y):
            @pl.when(rel == near)
            def _(near=near):
                finish_near(near, slot, first)

        @pl.when(rel == HERE)
        def _():
            for m in parts(first):
                total = part(total_of(HERE, slot), m, first)
                total[...] = total[...] + part(mine, m, first)[...]

    def left_half(block, kk, h):
        row = pl.multiple_of((far + kk) * BLK, BLK)
        val = dot(row, BLK, row, 2 * STRIP, pl.ds(pl.multiple_of(h * half, half), half))
        for m in range(2):
            block[rows_of(m, 0, BLK)] = (
                jnp.where(h > 0, block[rows_of(m, 0, BLK)], 0.0) + val[:, m * STRIP:(m + 1) * STRIP])

    def left_product(block, kk):
        row = pl.multiple_of((far + kk) * BLK, BLK)
        val = dot(row, BLK, row, 2 * STRIP)
        for m in range(2):
            block[rows_of(m, 0, BLK)] = val[:, m * STRIP:(m + 1) * STRIP]

    def corner_product(block, kk):
        row = pl.multiple_of((far + kk) * BLK + 2 * STRIP, STRIP)
        block[rows_of(2, 2 * STRIP, BLK)] = dot(row, STRIP, row, STRIP)

    def first_half(h, carry):
        load_half(h).wait()
        left_half(stage, 1 - core, h)
        return carry

    two, last = pl.ds(0, 2 * BLK), pl.ds(2 * BLK, BLK)
    first_total, next_total = total_of(DIAG, 0), total_of(DIAG, 1)
    copies = (
        pair_copy(part(stage, 0, True), part(first_total, 0, True), 0, 0),
        pair_copy(part(stage, 1, True), part(first_total, 1, True), 1, 1),
        pair_copy(part(stage, 2, True), part(first_total, 2, True), 2, 2),
        pair_copy(stage_next.at[two], next_total.at[two], 3, 3),
        pair_copy(stage_next.at[last], next_total.at[last], 4, 4),
    )

    lax.fori_loop(0, 2 * one, first_half, 0)
    pack_left(stage)
    pl.semaphore_wait(barrier, 3)
    copies[0].start()
    copies[1].start()
    load(1).wait()
    alone(lambda: left_product(mine, core))
    pack_left(mine)
    copies[0].wait_recv()
    finish_far(0, 0, True)
    copies[1].wait_recv()
    finish_far(0, 1, True)
    alone(lambda: corner_product(stage, 1 - core))
    pack_corner(stage)
    copies[2].start()
    load(2).wait()
    alone(lambda: product(stage_next, *block_rows(DIAG, 1, 1 - core), 0, 2))
    copies[3].start()
    alone(lambda: corner_product(mine, core))
    pack_corner(mine)
    copies[2].wait_recv()
    finish_far(0, 2, True)
    alone(lambda: product(mine, *block_rows(DIAG, 1, core), 0, 2))
    copies[3].wait_recv()
    finish_far(1, 0, False)
    finish_far(1, 1, False)
    alone(lambda: product(stage_next, *block_rows(DIAG, 1, 1 - core), 2, 1))
    copies[4].start()
    alone(lambda: product(mine, *block_rows(DIAG, 1, core), 2, 1))
    copies[4].wait_recv()
    finish_far(1, 2, False)
    finish_far(1, 3, False)
    for copy in copies:
        copy.wait_send()

    def body(step, carry):
        @pl.when(step < SLOTS + 1)
        def _():
            load(step + 1).wait()

        @pl.when(step == SLOTS)
        def _():
            load(GROUPS - 1).wait()

        rel, slot = step_task(step)

        @pl.when(exists(rel, slot))
        def _():
            product(stage, *block_rows(rel, slot, 1 - core))

            @pl.when(slot == 0)
            def _():
                pack_left(stage)
                pack_corner(stage)

            pair_block(step).start()
            product(mine, *block_rows(rel, slot, core))

            @pl.when(slot == 0)
            def _():
                pack_left(mine)
                pack_corner(mine)
                pair_block(step).wait_recv()
                finish(rel, slot, True)

            @pl.when(slot > 0)
            def _():
                pair_block(step).wait_recv()
                finish(rel, slot, False)

            pair_block(step).wait_send()

        return carry

    lax.fori_loop(2, STEPS, body, 0)

    def arrived(slot):
        first = slot == 0
        for ref, sem in ((from_x, fx_sem), (from_y, fy_sem)):
            whole = held(ref, slot).at[pl.ds(0, size(first))]
            pltpu.make_async_copy(whole, whole, sem.at[slot]).wait()
        for m in range(3):
            rows = pl.ds(*FIRST_PARTS[m]) if first else pl.ds(m * BLK, BLK)
            yield held(from_x, slot)[rows] + held(from_y, slot)[rows] + total_of(HERE, slot)[rows]

    unpack_symmetric(out_ref.at[0, 0], *arrived(0))
    for slot in range(1, SLOTS):
        @pl.when(exists(HERE, slot))
        def _(slot=slot):
            for m, total in enumerate(arrived(slot)):
                out_ref[0, slot, :, m * STRIP:(m + 1) * STRIP] = total

    @pl.when(jnp.logical_not(exists(HERE, SLOTS - 1)))
    def _():
        out_ref[0, SLOTS - 1] = jnp.zeros((BLK, BLK), jnp.float32)

    for rel in (DIAG, ALONG_X, ALONG_Y):
        for slots in (SLOTS - 1, SLOTS):
            @pl.when(exists(rel, SLOTS - 1) == (slots == SLOTS))
            def _(rel=rel, slots=slots):
                everything = acc.at[pl.ds(0, size(True) + (slots - 1) * ROWS)]
                pltpu.make_async_copy(everything, everything, send_sem.at[rel]).wait()


def solution(mesh):
    def local_gram(a_local):
        dma = pltpu.SemaphoreType.DMA

        def blocks(n):
            return pltpu.VMEM((n * ROWS, STRIP), jnp.float32)

        return pl.pallas_call(
            gram_kernel,
            out_shape=pltpu.VMEM((1, SLOTS, BLK, BLK), jnp.float32),
            in_specs=[pl.BlockSpec(memory_space=pl.ANY)],
            out_specs=pl.BlockSpec(memory_space=pltpu.VMEM),
            scratch_shapes=[
                pltpu.VMEM(a_local.shape, a_local.dtype),
                blocks(4 * SLOTS), blocks(1), blocks(1), blocks(1),
                blocks(SLOTS), blocks(SLOTS), blocks(SLOTS), blocks(SLOTS),
                dma((GROUPS + 1,)), dma((5,)), dma((8,)), dma((3,)),
                dma((SLOTS,)), dma((SLOTS,)), dma((SLOTS,)), dma((SLOTS,)),
            ],
            compiler_params=pltpu.CompilerParams(
                collective_id=0, has_side_effects=True, vmem_limit_bytes=56623104),
        )(a_local)

    return jax.shard_map(local_gram, mesh=mesh, in_specs=(P('mat', 'dp'),), out_specs=P(('mat', 'dp')), check_vma=False)
```

```python
import itertools

import jax
import jax.numpy as jnp
from jax import lax
from jax.experimental import pallas as pl
from jax.experimental.pallas import tpu as pltpu
from jax.sharding import PartitionSpec as P

MESH = pl.DeviceIdType.MESH
BLK = 384
STRIP = 128
ROWS = 3 * BLK
GROUPS = 8
SLOTS = 5
DIAG, ALONG_X, ALONG_Y, HERE = range(4)
STEPS = 4 * SLOTS - 1


def square(rows=STRIP):
    return (lax.broadcasted_iota(jnp.int32, (rows, STRIP), 0), lax.broadcasted_iota(jnp.int32, (rows, STRIP), 1))


FOLD = STRIP // 2
CORNER = FOLD + 8
FIRST_PARTS = ((0, BLK), (BLK, STRIP), (2 * BLK, CORNER))
CUT = 176
PARTS = ((0, BLK), (BLK, BLK), (2 * BLK, CUT), (2 * BLK + CUT, BLK - CUT))


def rows_of(m, start, stop):
    return slice(m * BLK + start, m * BLK + stop)


def pack_left(block):
    row, col = square()
    s11 = block[rows_of(1, STRIP, 2 * STRIP)]
    block[rows_of(0, 0, STRIP)] = jnp.where(row >= col, block[rows_of(0, 0, STRIP)], s11)
    block[rows_of(1, 0, STRIP)] = block[rows_of(1, 2 * STRIP, BLK)]
    main = jnp.sum(jnp.where(row == col, s11, 0.0), axis=0, keepdims=True)
    block[rows_of(2, FOLD, CORNER)] = jnp.where(square(8)[0] == 0, main, 0.0)


def pack_corner(block):
    row, col = square(FOLD)
    upper = block[rows_of(2, 2 * STRIP, 2 * STRIP + FOLD)]
    lower = block[rows_of(2, 2 * STRIP + FOLD, BLK)]
    main = jnp.sum(jnp.where(row == col, upper, 0.0), axis=0, keepdims=True)
    block[rows_of(2, 0, FOLD)] = jnp.where(col - FOLD > row, pltpu.roll(upper, FOLD, 1), lower)
    block[rows_of(2, FOLD, CORNER)] = jnp.where(square(8)[0] == 1, main, block[rows_of(2, FOLD, CORNER)])


def unpack_symmetric(ref, left, s21, corner):
    row, col = square()
    both, s10, s20 = left[0:STRIP], left[STRIP:2 * STRIP], left[2 * STRIP:]
    both_t = both.T
    fold = corner[0:FOLD]
    low = jnp.concatenate([pltpu.roll(fold, FOLD, 1), fold], axis=0)
    straight = jnp.where(jnp.maximum(row, col) >= FOLD, row - col, col - row) >= 0
    s22 = jnp.where(straight, low, low.T)
    ref[0:STRIP, 0:STRIP] = jnp.where(row >= col, both, both_t)
    ref[STRIP:2 * STRIP, STRIP:2 * STRIP] = jnp.where(
        row == col, corner[FOLD:FOLD + 1], jnp.where(row < col, both, both_t))
    ref[2 * STRIP:, 2 * STRIP:] = jnp.where(
        jnp.logical_and(row == col, row < FOLD), corner[FOLD + 1:FOLD + 2], s22)
    ref[STRIP:2 * STRIP, 0:STRIP] = s10
    ref[0:STRIP, STRIP:2 * STRIP] = s10.T
    ref[2 * STRIP:, 0:STRIP] = s20
    ref[0:STRIP, 2 * STRIP:] = s20.T
    ref[2 * STRIP:, STRIP:2 * STRIP] = s21
    ref[STRIP:2 * STRIP, 2 * STRIP:] = s21.T


def part(block, m, first):
    return block.at[pl.ds(*(FIRST_PARTS if first else PARTS)[m])]


def parts(first):
    return range(len(FIRST_PARTS if first else PARTS))


def size(first):
    return sum(rows for _, rows in FIRST_PARTS) if first else ROWS


def gram_kernel(a_hbm, out_ref, a_buf, acc, stage, stage_next, mine, from_x, from_y, relay_x, relay_y,
                load_sem, stage_sem, pair_sem, send_sem, fx_sem, fy_sem, rx_sem, ry_sem):
    me = lax.axis_index('dp')
    core = lax.rem(me, 2)
    x = lax.rem(me // 2, 2)
    y = me // 4
    half = a_buf.shape[1] // 2
    one = 1 + me // GROUPS

    def device(xx, yy, kk):
        return (yy * 2 + xx) * 2 + kk

    pair = device(x, y, 1 - core)
    nbr_x = device(1 - x, y, core)
    nbr_y = device(x, 1 - y, core)

    barrier = pltpu.get_barrier_semaphore()
    for other in (pair, nbr_x, nbr_y):
        pl.semaphore_signal(barrier, inc=1, device_id={'dp': other}, device_id_type=MESH)

    far = device(1 - x, 1 - y, 0)

    def load(n):
        row = far + core if isinstance(n, int) and n == 1 else lax.rem(far + 1 - n + GROUPS, GROUPS)
        rows = pl.ds(pl.multiple_of(row * BLK, BLK), BLK)
        return pltpu.make_async_copy(a_hbm.at[rows, :], a_buf.at[rows, :], load_sem.at[n])

    def load_half(h):
        rows = pl.ds(pl.multiple_of((far + 1 - core) * BLK, BLK), BLK)
        cols = pl.ds(pl.multiple_of(h * half, half), half)
        return pltpu.make_async_copy(a_hbm.at[rows, cols], a_buf.at[rows, cols], load_sem.at[GROUPS * h])

    load_half(0).start()
    load_half(1).start()
    for n in range(1, GROUPS):
        load(n).start()

    near_first = ALONG_X + y
    near_second = ALONG_Y - y

    def step_task(step):
        mid = step - SLOTS
        in_mid = jnp.logical_and(mid >= 0, mid < 2 * SLOTS - 1)
        to_first = jnp.logical_or(mid <= 0, lax.rem(mid + 2 * SLOTS, 2) == 1)
        near = jnp.where(to_first, near_first, near_second)
        near_slot = jnp.where(to_first, (mid + 1) // 2, mid // 2 - 1)
        rel = jnp.where(step < SLOTS, DIAG, jnp.where(in_mid, near, HERE))
        slot = jnp.where(step < SLOTS, step, jnp.where(in_mid, near_slot, step - 3 * SLOTS + 1))
        return rel, slot

    def dest_xy(rel):
        flip_x = jnp.where(rel <= ALONG_X, 1, 0)
        flip_y = jnp.where(lax.rem(rel, 2) == 0, 1, 0)
        xx = x + flip_x - 2 * flip_x * x
        yy = y + flip_y - 2 * flip_y * y
        return xx, yy

    def exists(rel, slot):
        _, yy = dest_xy(rel)
        return jnp.logical_or(slot < SLOTS - 1, yy == 0)

    def held(ref, slot):
        return ref.at[pl.ds(pl.multiple_of(slot * ROWS, ROWS), ROWS)]

    def total_of(rel, slot):
        return held(acc, rel * SLOTS + slot)

    def dot(left, left_rows, right, right_rows, cols=slice(None)):
        return lax.dot_general(a_buf[pl.ds(left, left_rows), cols], a_buf[pl.ds(right, right_rows), cols],
                               (((1,), (1,)), ((), ())), preferred_element_type=jnp.float32)

    def block_rows(rel, slot, kk):
        xx, yy = dest_xy(rel)
        p = device(xx, yy, kk)
        q = lax.rem(p - slot + GROUPS, GROUPS)
        hi = pl.multiple_of(jnp.maximum(p, q) * BLK, BLK)
        lo = pl.multiple_of(jnp.minimum(p, q) * BLK, BLK)
        return hi, lo

    def product(block, hi, lo, first=0, count=3):
        val = dot(hi, BLK, lo + first * STRIP, count * STRIP)
        for m in range(count):
            block[rows_of(first + m, 0, BLK)] = val[:, m * STRIP:(m + 1) * STRIP]

    def alone(work):
        def run(_, carry):
            work()
            return carry

        lax.fori_loop(0, one, run, 0)

    def pair_copy(src, dst, send, recv):
        return pltpu.make_async_remote_copy(
            src_ref=src, dst_ref=dst, send_sem=stage_sem.at[send], recv_sem=pair_sem.at[recv],
            device_id={'dp': pair}, device_id_type=MESH)

    def pair_block(step):
        return pair_copy(stage, total_of(*step_task(step)), 0, 5 + lax.rem(step, 3))

    def by_y(slot, m, first, dest_x, dest_y):
        if first:
            return (core if m == 0 else 1 - core) == 1

        def listed(*bits):
            return jnp.where(slot == 1, bits[0], jnp.where(slot == 2, bits[1], jnp.where(slot == 3, bits[2], bits[3])))

        to_zero = jnp.where(core == 0, listed(13, 2, 1, 1), listed(1, 1, 2, 2))
        to_one = jnp.where(core == 0, listed(5, 2, 1, 4), listed(5, 1, 2, 2))
        bits = jnp.where(dest_y == 1, 13, jnp.where(dest_x == 0, to_zero, to_one))
        return lax.rem(bits // 2 ** m, 2) == 1

    def relay_wait(slot, first, relay, sem, flags):
        each = [part_rows for _, part_rows in (FIRST_PARTS if first else PARTS)]
        rows = sum(jnp.where(flag, part_rows, 0) for flag, part_rows in zip(flags, each))
        possible = {sum(chosen) for n in range(1, len(each) + 1) for chosen in itertools.combinations(each, n)}
        for count in sorted(possible):
            @pl.when(rows == count)
            def _(count=count):
                whole = held(relay, slot).at[pl.ds(0, count)]
                pltpu.make_async_copy(whole, whole, sem.at[slot]).wait()

    def far_send(slot, m, first, along_y):
        return pltpu.make_async_remote_copy(
            src_ref=part(total_of(DIAG, slot), m, first),
            dst_ref=part(held(relay_x if along_y else relay_y, slot), m, first),
            send_sem=send_sem.at[DIAG],
            recv_sem=(rx_sem if along_y else ry_sem).at[slot],
            device_id={'dp': nbr_y if along_y else nbr_x}, device_id_type=MESH)

    def near_send(rel, slot, m, first):
        along_y = rel == ALONG_Y
        return pltpu.make_async_remote_copy(
            src_ref=part(total_of(rel, slot), m, first),
            dst_ref=part(held(from_y if along_y else from_x, slot), m, first),
            send_sem=send_sem.at[rel],
            recv_sem=(fy_sem if along_y else fx_sem).at[slot],
            device_id={'dp': nbr_y if along_y else nbr_x}, device_id_type=MESH)

    def finish_far(slot, m, first):
        total = part(total_of(DIAG, slot), m, first)
        total[...] = total[...] + part(mine, m, first)[...]
        along_y = by_y(slot, m, first, 1 - x, 1 - y)

        @pl.when(along_y)
        def _():
            far_send(slot, m, first, True).start()

        @pl.when(jnp.logical_not(along_y))
        def _():
            far_send(slot, m, first, False).start()

    def finish_near(rel, slot, first):
        if rel == ALONG_X:
            relay, sem = relay_x, rx_sem
            flags = [by_y(slot, m, first, 1 - x, y) for m in parts(first)]
        else:
            relay, sem = relay_y, ry_sem
            flags = [jnp.logical_not(by_y(slot, m, first, x, 1 - y)) for m in parts(first)]
        relay_wait(slot, first, relay, sem, flags)
        for m in parts(first):
            total = part(total_of(rel, slot), m, first)

            @pl.when(flags[m])
            def _(m=m, total=total):
                total[...] = total[...] + part(mine, m, first)[...] + part(held(relay, slot), m, first)[...]

            @pl.when(jnp.logical_not(flags[m]))
            def _(m=m, total=total):
                total[...] = total[...] + part(mine, m, first)[...]

            near_send(rel, slot, m, first).start()

    def finish(rel, slot, first):
        @pl.when(rel == DIAG)
        def _():
            for m in parts(first):
                finish_far(slot, m, first)

        for near in (ALONG_X, ALONG_Y):
            @pl.when(rel == near)
            def _(near=near):
                finish_near(near, slot, first)

        @pl.when(rel == HERE)
        def _():
            for m in parts(first):
                total = part(total_of(HERE, slot), m, first)
                total[...] = total[...] + part(mine, m, first)[...]

    def left_half(block, kk, h):
        row = pl.multiple_of((far + kk) * BLK, BLK)
        val = dot(row, BLK, row, 2 * STRIP, pl.ds(pl.multiple_of(h * half, half), half))
        for m in range(2):
            block[rows_of(m, 0, BLK)] = (
                jnp.where(h > 0, block[rows_of(m, 0, BLK)], 0.0) + val[:, m * STRIP:(m + 1) * STRIP])

    def left_product(block, kk):
        row = pl.multiple_of((far + kk) * BLK, BLK)
        val = dot(row, BLK, row, 2 * STRIP)
        for m in range(2):
            block[rows_of(m, 0, BLK)] = val[:, m * STRIP:(m + 1) * STRIP]

    def corner_product(block, kk):
        row = pl.multiple_of((far + kk) * BLK + 2 * STRIP, STRIP)
        block[rows_of(2, 2 * STRIP, BLK)] = dot(row, STRIP, row, STRIP)

    def first_half(h, carry):
        load_half(h).wait()
        left_half(stage, 1 - core, h)
        return carry

    two, last = pl.ds(0, 2 * BLK), pl.ds(2 * BLK, BLK)
    first_total, next_total = total_of(DIAG, 0), total_of(DIAG, 1)
    copies = (
        pair_copy(part(stage, 0, True), part(first_total, 0, True), 0, 0),
        pair_copy(part(stage, 1, True), part(first_total, 1, True), 1, 1),
        pair_copy(part(stage, 2, True), part(first_total, 2, True), 2, 2),
        pair_copy(stage_next.at[two], next_total.at[two], 3, 3),
        pair_copy(stage_next.at[last], next_total.at[last], 4, 4),
    )

    lax.fori_loop(0, 2 * one, first_half, 0)
    pack_left(stage)
    pl.semaphore_wait(barrier, 3)
    copies[0].start()
    copies[1].start()
    load(1).wait()
    alone(lambda: left_product(mine, core))
    pack_left(mine)
    copies[0].wait_recv()
    finish_far(0, 0, True)
    copies[1].wait_recv()
    finish_far(0, 1, True)
    alone(lambda: corner_product(stage, 1 - core))
    pack_corner(stage)
    copies[2].start()
    load(2).wait()
    alone(lambda: product(stage_next, *block_rows(DIAG, 1, 1 - core), 0, 2))
    copies[3].start()
    alone(lambda: corner_product(mine, core))
    pack_corner(mine)
    copies[2].wait_recv()
    finish_far(0, 2, True)
    alone(lambda: product(mine, *block_rows(DIAG, 1, core), 0, 2))
    copies[3].wait_recv()
    finish_far(1, 0, False)
    finish_far(1, 1, False)
    alone(lambda: product(stage_next, *block_rows(DIAG, 1, 1 - core), 2, 1))
    copies[4].start()
    alone(lambda: product(mine, *block_rows(DIAG, 1, core), 2, 1))
    copies[4].wait_recv()
    finish_far(1, 2, False)
    finish_far(1, 3, False)
    for copy in copies:
        copy.wait_send()

    def body(step, carry):
        @pl.when(step < SLOTS + 1)
        def _():
            load(step + 1).wait()

        @pl.when(step == SLOTS)
        def _():
            load(GROUPS - 1).wait()

        rel, slot = step_task(step)

        @pl.when(exists(rel, slot))
        def _():
            product(stage, *block_rows(rel, slot, 1 - core))

            @pl.when(slot == 0)
            def _():
                pack_left(stage)
                pack_corner(stage)

            pair_block(step).start()
            product(mine, *block_rows(rel, slot, core))

            @pl.when(slot == 0)
            def _():
                pack_left(mine)
                pack_corner(mine)
                pair_block(step).wait_recv()
                finish(rel, slot, True)

            @pl.when(slot > 0)
            def _():
                pair_block(step).wait_recv()
                finish(rel, slot, False)

            pair_block(step).wait_send()

        return carry

    lax.fori_loop(2, STEPS, body, 0)

    def arrived(slot):
        first = slot == 0
        for ref, sem in ((from_x, fx_sem), (from_y, fy_sem)):
            whole = held(ref, slot).at[pl.ds(0, size(first))]
            pltpu.make_async_copy(whole, whole, sem.at[slot]).wait()
        for m in range(3):
            rows = pl.ds(*FIRST_PARTS[m]) if first else pl.ds(m * BLK, BLK)
            yield held(from_x, slot)[rows] + held(from_y, slot)[rows] + total_of(HERE, slot)[rows]

    unpack_symmetric(out_ref.at[0, 0], *arrived(0))
    for slot in range(1, SLOTS):
        @pl.when(exists(HERE, slot))
        def _(slot=slot):
            for m, total in enumerate(arrived(slot)):
                out_ref[0, slot, :, m * STRIP:(m + 1) * STRIP] = total

    @pl.when(jnp.logical_not(exists(HERE, SLOTS - 1)))
    def _():
        out_ref[0, SLOTS - 1] = jnp.zeros((BLK, BLK), jnp.float32)

    for rel in (DIAG, ALONG_X, ALONG_Y):
        for slots in (SLOTS - 1, SLOTS):
            @pl.when(exists(rel, SLOTS - 1) == (slots == SLOTS))
            def _(rel=rel, slots=slots):
                everything = acc.at[pl.ds(0, size(True) + (slots - 1) * ROWS)]
                pltpu.make_async_copy(everything, everything, send_sem.at[rel]).wait()


def solution(mesh):
    def local_gram(a_local):
        dma = pltpu.SemaphoreType.DMA

        def blocks(n):
            return pltpu.VMEM((n * ROWS, STRIP), jnp.float32)

        return pl.pallas_call(
            gram_kernel,
            out_shape=pltpu.VMEM((1, SLOTS, BLK, BLK), jnp.float32),
            in_specs=[pl.BlockSpec(memory_space=pl.ANY)],
            out_specs=pl.BlockSpec(memory_space=pltpu.VMEM),
            scratch_shapes=[
                pltpu.VMEM(a_local.shape, a_local.dtype),
                blocks(4 * SLOTS), blocks(1), blocks(1), blocks(1),
                blocks(SLOTS), blocks(SLOTS), blocks(SLOTS), blocks(SLOTS),
                dma((GROUPS + 1,)), dma((5,)), dma((8,)), dma((3,)),
                dma((SLOTS,)), dma((SLOTS,)), dma((SLOTS,)), dma((SLOTS,)),
            ],
            compiler_params=pltpu.CompilerParams(
                collective_id=0, has_side_effects=True, vmem_limit_bytes=56623104),
        )(a_local)

    return jax.shard_map(local_gram, mesh=mesh, in_specs=(P('mat', 'dp'),), out_specs=P(('mat', 'dp')), check_vma=False)
```

```python
import itertools

import jax
import jax.numpy as jnp
from jax import lax
from jax.experimental import pallas as pl
from jax.experimental.pallas import tpu as pltpu
from jax.sharding import PartitionSpec as P

MESH = pl.DeviceIdType.MESH
BLK = 384
STRIP = 128
ROWS = 3 * BLK
GROUPS = 8
SLOTS = 5
DIAG, ALONG_X, ALONG_Y, HERE = range(4)
STEPS = 4 * SLOTS - 1


def square(rows=STRIP):
    return (lax.broadcasted_iota(jnp.int32, (rows, STRIP), 0), lax.broadcasted_iota(jnp.int32, (rows, STRIP), 1))


FOLD = STRIP // 2
CORNER = FOLD + 8
FIRST_PARTS = ((0, BLK), (BLK, STRIP), (2 * BLK, CORNER))
CUT = 176
PARTS = ((0, BLK), (BLK, BLK), (2 * BLK, CUT), (2 * BLK + CUT, BLK - CUT))


def rows_of(m, start, stop):
    return slice(m * BLK + start, m * BLK + stop)


def pack_left(block):
    row, col = square()
    s11 = block[rows_of(1, STRIP, 2 * STRIP)]
    block[rows_of(0, 0, STRIP)] = jnp.where(row >= col, block[rows_of(0, 0, STRIP)], s11)
    block[rows_of(1, 0, STRIP)] = block[rows_of(1, 2 * STRIP, BLK)]
    main = jnp.sum(jnp.where(row == col, s11, 0.0), axis=0, keepdims=True)
    block[rows_of(2, FOLD, CORNER)] = jnp.where(square(8)[0] == 0, main, 0.0)


def pack_corner(block):
    row, col = square(FOLD)
    upper = block[rows_of(2, 2 * STRIP, 2 * STRIP + FOLD)]
    lower = block[rows_of(2, 2 * STRIP + FOLD, BLK)]
    main = jnp.sum(jnp.where(row == col, upper, 0.0), axis=0, keepdims=True)
    block[rows_of(2, 0, FOLD)] = jnp.where(col - FOLD > row, pltpu.roll(upper, FOLD, 1), lower)
    block[rows_of(2, FOLD, CORNER)] = jnp.where(square(8)[0] == 1, main, block[rows_of(2, FOLD, CORNER)])


def unpack_symmetric(ref, left, s21, corner):
    row, col = square()
    both, s10, s20 = left[0:STRIP], left[STRIP:2 * STRIP], left[2 * STRIP:]
    both_t = both.T
    fold = corner[0:FOLD]
    low = jnp.concatenate([pltpu.roll(fold, FOLD, 1), fold], axis=0)
    straight = jnp.where(jnp.maximum(row, col) >= FOLD, row - col, col - row) >= 0
    s22 = jnp.where(straight, low, low.T)
    ref[0:STRIP, 0:STRIP] = jnp.where(row >= col, both, both_t)
    ref[STRIP:2 * STRIP, STRIP:2 * STRIP] = jnp.where(
        row == col, corner[FOLD:FOLD + 1], jnp.where(row < col, both, both_t))
    ref[2 * STRIP:, 2 * STRIP:] = jnp.where(
        jnp.logical_and(row == col, row < FOLD), corner[FOLD + 1:FOLD + 2], s22)
    ref[STRIP:2 * STRIP, 0:STRIP] = s10
    ref[0:STRIP, STRIP:2 * STRIP] = s10.T
    ref[2 * STRIP:, 0:STRIP] = s20
    ref[0:STRIP, 2 * STRIP:] = s20.T
    ref[2 * STRIP:, STRIP:2 * STRIP] = s21
    ref[STRIP:2 * STRIP, 2 * STRIP:] = s21.T


def part(block, m, first):
    return block.at[pl.ds(*(FIRST_PARTS if first else PARTS)[m])]


def parts(first):
    return range(len(FIRST_PARTS if first else PARTS))


def size(first):
    return sum(rows for _, rows in FIRST_PARTS) if first else ROWS


def gram_kernel(a_hbm, out_ref, a_buf, acc, stage, stage_next, mine, from_x, from_y, relay_x, relay_y,
                load_sem, stage_sem, pair_sem, send_sem, from_sem, rx_sem, ry_sem):
    me = lax.axis_index('dp')
    core = lax.rem(me, 2)
    x = lax.rem(me // 2, 2)
    y = me // 4
    half = a_buf.shape[1] // 2
    one = 1 + me // GROUPS

    def device(xx, yy, kk):
        return (yy * 2 + xx) * 2 + kk

    pair = device(x, y, 1 - core)
    nbr_x = device(1 - x, y, core)
    nbr_y = device(x, 1 - y, core)

    barrier = pltpu.get_barrier_semaphore()
    for other in (pair, nbr_x, nbr_y):
        pl.semaphore_signal(barrier, inc=1, device_id={'dp': other}, device_id_type=MESH)

    far = device(1 - x, 1 - y, 0)

    def load(n):
        row = far + core if n == 1 else lax.rem(far + 1 - n + GROUPS, GROUPS)
        rows = pl.ds(pl.multiple_of(row * BLK, BLK), BLK)
        return pltpu.make_async_copy(a_hbm.at[rows, :], a_buf.at[rows, :], load_sem.at[min(n, 3)])

    def load_half(h):
        rows = pl.ds(pl.multiple_of((far + 1 - core) * BLK, BLK), BLK)
        cols = pl.ds(pl.multiple_of(h * half, half), half)
        return pltpu.make_async_copy(a_hbm.at[rows, cols], a_buf.at[rows, cols], load_sem.at[4 * h])

    load_half(0).start()
    load_half(1).start()
    for n in range(1, GROUPS):
        load(n).start()

    near_first = ALONG_X + y
    near_second = ALONG_Y - y

    def step_task(step):
        mid = step - SLOTS
        in_mid = jnp.logical_and(mid >= 0, mid < 2 * SLOTS - 1)
        to_first = jnp.logical_or(mid <= 0, lax.rem(mid + 2 * SLOTS, 2) == 1)
        near = jnp.where(to_first, near_first, near_second)
        near_slot = jnp.where(to_first, (mid + 1) // 2, mid // 2 - 1)
        rel = jnp.where(step < SLOTS, DIAG, jnp.where(in_mid, near, HERE))
        slot = jnp.where(step < SLOTS, step, jnp.where(in_mid, near_slot, step - 3 * SLOTS + 1))
        return rel, slot

    def dest_xy(rel):
        flip_x = jnp.where(rel <= ALONG_X, 1, 0)
        flip_y = jnp.where(lax.rem(rel, 2) == 0, 1, 0)
        xx = x + flip_x - 2 * flip_x * x
        yy = y + flip_y - 2 * flip_y * y
        return xx, yy

    def exists(rel, slot):
        _, yy = dest_xy(rel)
        return jnp.logical_or(slot < SLOTS - 1, yy == 0)

    def held(ref, slot):
        return ref.at[pl.ds(pl.multiple_of(slot * ROWS, ROWS), ROWS)]

    def total_of(rel, slot):
        return held(acc, rel * SLOTS + slot)

    def dot(left, left_rows, right, right_rows, cols=slice(None)):
        return lax.dot_general(a_buf[pl.ds(left, left_rows), cols], a_buf[pl.ds(right, right_rows), cols],
                               (((1,), (1,)), ((), ())), preferred_element_type=jnp.float32)

    def block_rows(rel, slot, kk):
        xx, yy = dest_xy(rel)
        p = device(xx, yy, kk)
        q = lax.rem(p - slot + GROUPS, GROUPS)
        hi = pl.multiple_of(jnp.maximum(p, q) * BLK, BLK)
        lo = pl.multiple_of(jnp.minimum(p, q) * BLK, BLK)
        return hi, lo

    def product(block, hi, lo, first=0, count=3):
        val = dot(hi, BLK, lo + first * STRIP, count * STRIP)
        for m in range(count):
            block[rows_of(first + m, 0, BLK)] = val[:, m * STRIP:(m + 1) * STRIP]

    def alone(work):
        def run(_, carry):
            work()
            return carry

        lax.fori_loop(0, one, run, 0)

    def pair_copy(src, dst, recv):
        return pltpu.make_async_remote_copy(
            src_ref=src, dst_ref=dst, send_sem=stage_sem, recv_sem=pair_sem.at[recv],
            device_id={'dp': pair}, device_id_type=MESH)

    def pair_block(step):
        return pair_copy(stage, total_of(*step_task(step)), 3 + lax.rem(step + 1, 3))

    def by_y(slot, m, first, dest_x, dest_y):
        if first:
            return (core if m == 0 else 1 - core) == 1

        def listed(*bits):
            return jnp.where(slot == 1, bits[0], jnp.where(slot == 2, bits[1], jnp.where(slot == 3, bits[2], bits[3])))

        to_zero = jnp.where(core == 0, listed(13, 2, 1, 1), listed(1, 1, 2, 2))
        to_one = jnp.where(core == 0, listed(5, 2, 1, 4), listed(5, 1, 2, 2))
        bits = jnp.where(dest_y == 1, 13, jnp.where(dest_x == 0, to_zero, to_one))
        return lax.rem(bits // 2 ** m, 2) == 1

    def relay_wait(slot, first, relay, sem, flags):
        each = [part_rows for _, part_rows in (FIRST_PARTS if first else PARTS)]
        rows = sum(jnp.where(flag, part_rows, 0) for flag, part_rows in zip(flags, each))
        possible = {sum(chosen) for n in range(1, len(each) + 1) for chosen in itertools.combinations(each, n)}
        for count in sorted(possible):
            @pl.when(rows == count)
            def _(count=count):
                whole = held(relay, slot).at[pl.ds(0, count)]
                pltpu.make_async_copy(whole, whole, sem.at[slot]).wait()

    def far_send(slot, m, first, along_y):
        return pltpu.make_async_remote_copy(
            src_ref=part(total_of(DIAG, slot), m, first),
            dst_ref=part(held(relay_x if along_y else relay_y, slot), m, first),
            send_sem=send_sem,
            recv_sem=(rx_sem if along_y else ry_sem).at[slot],
            device_id={'dp': nbr_y if along_y else nbr_x}, device_id_type=MESH)

    def near_send(rel, slot, m, first):
        along_y = rel == ALONG_Y
        return pltpu.make_async_remote_copy(
            src_ref=part(total_of(rel, slot), m, first),
            dst_ref=part(held(from_y if along_y else from_x, slot), m, first),
            send_sem=send_sem,
            recv_sem=from_sem.at[slot],
            device_id={'dp': nbr_y if along_y else nbr_x}, device_id_type=MESH)

    def finish_far(slot, m, first):
        total = part(total_of(DIAG, slot), m, first)
        total[...] = total[...] + part(mine, m, first)[...]
        along_y = by_y(slot, m, first, 1 - x, 1 - y)

        @pl.when(along_y)
        def _():
            far_send(slot, m, first, True).start()

        @pl.when(jnp.logical_not(along_y))
        def _():
            far_send(slot, m, first, False).start()

    def finish_near(rel, slot, first):
        if rel == ALONG_X:
            relay, sem = relay_x, rx_sem
            flags = [by_y(slot, m, first, 1 - x, y) for m in parts(first)]
        else:
            relay, sem = relay_y, ry_sem
            flags = [jnp.logical_not(by_y(slot, m, first, x, 1 - y)) for m in parts(first)]
        relay_wait(slot, first, relay, sem, flags)
        for m in parts(first):
            total = part(total_of(rel, slot), m, first)

            @pl.when(flags[m])
            def _(m=m, total=total):
                total[...] = total[...] + part(mine, m, first)[...] + part(held(relay, slot), m, first)[...]

            @pl.when(jnp.logical_not(flags[m]))
            def _(m=m, total=total):
                total[...] = total[...] + part(mine, m, first)[...]

            near_send(rel, slot, m, first).start()

    def finish(rel, slot, first):
        @pl.when(rel == DIAG)
        def _():
            for m in parts(first):
                finish_far(slot, m, first)

        for near in (ALONG_X, ALONG_Y):
            @pl.when(rel == near)
            def _(near=near):
                finish_near(near, slot, first)

        @pl.when(rel == HERE)
        def _():
            for m in parts(first):
                total = part(total_of(HERE, slot), m, first)
                total[...] = total[...] + part(mine, m, first)[...]

    def left_half(block, kk, h):
        row = pl.multiple_of((far + kk) * BLK, BLK)
        val = dot(row, BLK, row, 2 * STRIP, pl.ds(pl.multiple_of(h * half, half), half))
        for m in range(2):
            block[rows_of(m, 0, BLK)] = (
                jnp.where(h > 0, block[rows_of(m, 0, BLK)], 0.0) + val[:, m * STRIP:(m + 1) * STRIP])

    def left_product(block, kk):
        row = pl.multiple_of((far + kk) * BLK, BLK)
        val = dot(row, BLK, row, 2 * STRIP)
        for m in range(2):
            block[rows_of(m, 0, BLK)] = val[:, m * STRIP:(m + 1) * STRIP]

    def corner_product(block, kk):
        row = pl.multiple_of((far + kk) * BLK + 2 * STRIP, STRIP)
        block[rows_of(2, 2 * STRIP, BLK)] = dot(row, STRIP, row, STRIP)

    def first_half(h, carry):
        load_half(h).wait()
        left_half(stage, 1 - core, h)
        return carry

    two, last = pl.ds(0, 2 * BLK), pl.ds(2 * BLK, BLK)
    first_total, next_total = total_of(DIAG, 0), total_of(DIAG, 1)
    copies = (
        pair_copy(part(stage, 0, True), part(first_total, 0, True), 0),
        pair_copy(part(stage, 1, True), part(first_total, 1, True), 1),
        pair_copy(part(stage, 2, True), part(first_total, 2, True), 2),
        pair_copy(stage_next.at[two], next_total.at[two], 4),
        pair_copy(stage_next.at[last], next_total.at[last], 5),
    )

    lax.fori_loop(0, 2 * one, first_half, 0)
    pack_left(stage)
    pl.semaphore_wait(barrier, 3)
    copies[0].start()
    copies[1].start()
    load(1).wait()
    alone(lambda: left_product(mine, core))
    pack_left(mine)
    copies[0].wait_recv()
    finish_far(0, 0, True)
    copies[1].wait_recv()
    finish_far(0, 1, True)
    alone(lambda: corner_product(stage, 1 - core))
    pack_corner(stage)
    copies[2].start()
    load(2).wait()
    alone(lambda: product(stage_next, *block_rows(DIAG, 1, 1 - core), 0, 2))
    copies[3].start()
    alone(lambda: corner_product(mine, core))
    pack_corner(mine)
    copies[2].wait_recv()
    finish_far(0, 2, True)
    alone(lambda: product(mine, *block_rows(DIAG, 1, core), 0, 2))
    copies[3].wait_recv()
    finish_far(1, 0, False)
    finish_far(1, 1, False)
    alone(lambda: product(stage_next, *block_rows(DIAG, 1, 1 - core), 2, 1))
    copies[4].start()
    alone(lambda: product(mine, *block_rows(DIAG, 1, core), 2, 1))
    copies[4].wait_recv()
    finish_far(1, 2, False)
    finish_far(1, 3, False)
    both = acc.at[pl.ds(0, size(True) + ROWS)]
    pltpu.make_async_copy(both, both, stage_sem).wait()

    def body(step, carry):
        @pl.when(step == 2)
        def _():
            rest = pl.ds(0, (GROUPS - 3) * BLK)
            pltpu.make_async_copy(a_hbm.at[rest, :], a_buf.at[rest, :], load_sem.at[3]).wait()

        rel, slot = step_task(step)

        @pl.when(exists(rel, slot))
        def _():
            product(stage, *block_rows(rel, slot, 1 - core))

            @pl.when(slot == 0)
            def _():
                pack_left(stage)
                pack_corner(stage)

            pair_block(step).start()
            product(mine, *block_rows(rel, slot, core))

            @pl.when(slot == 0)
            def _():
                pack_left(mine)
                pack_corner(mine)
                pair_block(step).wait_recv()
                finish(rel, slot, True)

            @pl.when(slot > 0)
            def _():
                pair_block(step).wait_recv()
                finish(rel, slot, False)

            pair_block(step).wait_send()

        return carry

    lax.fori_loop(2, STEPS, body, 0)

    def arrived(slot):
        first = slot == 0
        two_of = acc.at[pl.ds(0, 2 * size(first))]
        pltpu.make_async_copy(two_of, two_of, from_sem.at[slot]).wait()
        for m in range(3):
            rows = pl.ds(*FIRST_PARTS[m]) if first else pl.ds(m * BLK, BLK)
            yield held(from_x, slot)[rows] + held(from_y, slot)[rows] + total_of(HERE, slot)[rows]

    unpack_symmetric(out_ref.at[0, 0], *arrived(0))
    for slot in range(1, SLOTS):
        @pl.when(exists(HERE, slot))
        def _(slot=slot):
            for m, total in enumerate(arrived(slot)):
                out_ref[0, slot, :, m * STRIP:(m + 1) * STRIP] = total

    @pl.when(jnp.logical_not(exists(HERE, SLOTS - 1)))
    def _():
        out_ref[0, SLOTS - 1] = jnp.zeros((BLK, BLK), jnp.float32)

    for longer in (1, 2):
        @pl.when(y == longer - 1)
        def _(longer=longer):
            everything = acc.at[pl.ds(0, 3 * size(True) + (3 * (SLOTS - 2) + longer) * ROWS)]
            pltpu.make_async_copy(everything, everything, send_sem).wait()


def solution(mesh):
    def local_gram(a_local):
        dma = pltpu.SemaphoreType.DMA

        def blocks(n):
            return pltpu.VMEM((n * ROWS, STRIP), jnp.float32)

        return pl.pallas_call(
            gram_kernel,
            out_shape=pltpu.VMEM((1, SLOTS, BLK, BLK), jnp.float32),
            in_specs=[pl.BlockSpec(memory_space=pl.ANY)],
            out_specs=pl.BlockSpec(memory_space=pltpu.VMEM),
            scratch_shapes=[
                pltpu.VMEM(a_local.shape, a_local.dtype),
                blocks(4 * SLOTS), blocks(1), blocks(1), blocks(1),
                blocks(SLOTS), blocks(SLOTS), blocks(SLOTS), blocks(SLOTS),
                dma((5,)), dma, dma((6,)), dma, dma((SLOTS,)), dma((SLOTS,)), dma((SLOTS,)),
            ],
            compiler_params=pltpu.CompilerParams(
                collective_id=0, has_side_effects=True, vmem_limit_bytes=56623104),
        )(a_local)

    return jax.shard_map(local_gram, mesh=mesh, in_specs=(P('mat', 'dp'),), out_specs=P(('mat', 'dp')), check_vma=False)
```

```python
import itertools

import jax
import jax.numpy as jnp
from jax import lax
from jax.experimental import pallas as pl
from jax.experimental.pallas import tpu as pltpu
from jax.sharding import PartitionSpec as P

MESH = pl.DeviceIdType.MESH
BLK = 384
STRIP = 128
ROWS = 3 * BLK
GROUPS = 8
SLOTS = 5
DIAG, ALONG_X, ALONG_Y, HERE = range(4)
STEPS = 4 * SLOTS - 1


def square(rows=STRIP):
    return (lax.broadcasted_iota(jnp.int32, (rows, STRIP), 0), lax.broadcasted_iota(jnp.int32, (rows, STRIP), 1))


FOLD = STRIP // 2
CORNER = FOLD + 8
FIRST_PARTS = ((0, BLK), (BLK, STRIP), (2 * BLK, CORNER))
CUT = 176
PARTS = ((0, BLK), (BLK, BLK), (2 * BLK, CUT), (2 * BLK + CUT, BLK - CUT))


def rows_of(m, start, stop):
    return slice(m * BLK + start, m * BLK + stop)


def pack_left(block):
    row, col = square()
    s11 = block[rows_of(1, STRIP, 2 * STRIP)]
    block[rows_of(0, 0, STRIP)] = jnp.where(row >= col, block[rows_of(0, 0, STRIP)], s11)
    block[rows_of(1, 0, STRIP)] = block[rows_of(1, 2 * STRIP, BLK)]
    main = jnp.sum(jnp.where(row == col, s11, 0.0), axis=0, keepdims=True)
    block[rows_of(2, FOLD, CORNER)] = jnp.where(square(8)[0] == 0, main, 0.0)


def pack_corner(block):
    row, col = square(FOLD)
    upper = block[rows_of(2, 2 * STRIP, 2 * STRIP + FOLD)]
    lower = block[rows_of(2, 2 * STRIP + FOLD, BLK)]
    main = jnp.sum(jnp.where(row == col, upper, 0.0), axis=0, keepdims=True)
    block[rows_of(2, 0, FOLD)] = jnp.where(col - FOLD > row, pltpu.roll(upper, FOLD, 1), lower)
    block[rows_of(2, FOLD, CORNER)] = jnp.where(square(8)[0] == 1, main, block[rows_of(2, FOLD, CORNER)])


def unpack_symmetric(ref, left, s21, corner):
    row, col = square()
    both, s10, s20 = left[0:STRIP], left[STRIP:2 * STRIP], left[2 * STRIP:]
    both_t = both.T
    fold = corner[0:FOLD]
    low = jnp.concatenate([pltpu.roll(fold, FOLD, 1), fold], axis=0)
    straight = jnp.where(jnp.maximum(row, col) >= FOLD, row - col, col - row) >= 0
    s22 = jnp.where(straight, low, low.T)
    ref[0:STRIP, 0:STRIP] = jnp.where(row >= col, both, both_t)
    ref[STRIP:2 * STRIP, STRIP:2 * STRIP] = jnp.where(
        row == col, corner[FOLD:FOLD + 1], jnp.where(row < col, both, both_t))
    ref[2 * STRIP:, 2 * STRIP:] = jnp.where(
        jnp.logical_and(row == col, row < FOLD), corner[FOLD + 1:FOLD + 2], s22)
    ref[STRIP:2 * STRIP, 0:STRIP] = s10
    ref[0:STRIP, STRIP:2 * STRIP] = s10.T
    ref[2 * STRIP:, 0:STRIP] = s20
    ref[0:STRIP, 2 * STRIP:] = s20.T
    ref[2 * STRIP:, STRIP:2 * STRIP] = s21
    ref[STRIP:2 * STRIP, 2 * STRIP:] = s21.T


def part(block, m, first):
    return block.at[pl.ds(*(FIRST_PARTS if first else PARTS)[m])]


def parts(first):
    return range(len(FIRST_PARTS if first else PARTS))


def size(first):
    return sum(rows for _, rows in FIRST_PARTS) if first else ROWS


def gram_kernel(a_hbm, out_ref, a_buf, acc, stage, stage_next, mine, from_x, from_y, relay_x, relay_y,
                load_sem, stage_sem, pair_sem, send_sem, from_sem, rx_sem, ry_sem):
    me = lax.axis_index('dp')
    core = lax.rem(me, 2)
    x = lax.rem(me // 2, 2)
    y = me // 4
    half = a_buf.shape[1] // 2
    one = 1 + me // GROUPS

    def device(xx, yy, kk):
        return (yy * 2 + xx) * 2 + kk

    pair = device(x, y, 1 - core)
    nbr_x = device(1 - x, y, core)
    nbr_y = device(x, 1 - y, core)

    barrier = pltpu.get_barrier_semaphore()
    for other in (pair, nbr_x, nbr_y):
        pl.semaphore_signal(barrier, inc=1, device_id={'dp': other}, device_id_type=MESH)

    far = device(1 - x, 1 - y, 0)

    def load(n):
        row = far + core if n == 1 else lax.rem(far + 1 - n + GROUPS, GROUPS)
        rows = pl.ds(pl.multiple_of(row * BLK, BLK), BLK)
        return pltpu.make_async_copy(a_hbm.at[rows, :], a_buf.at[rows, :], load_sem.at[min(n, 3)])

    def load_half(h):
        rows = pl.ds(pl.multiple_of((far + 1 - core) * BLK, BLK), BLK)
        cols = pl.ds(pl.multiple_of(h * half, half), half)
        return pltpu.make_async_copy(a_hbm.at[rows, cols], a_buf.at[rows, cols], load_sem.at[4 * h])

    load_half(0).start()
    load_half(1).start()
    for n in range(1, GROUPS):
        load(n).start()

    near_first = ALONG_X + y
    near_second = ALONG_Y - y

    def step_task(step):
        mid = step - SLOTS
        in_mid = jnp.logical_and(mid >= 0, mid < 2 * SLOTS - 1)
        to_first = jnp.logical_or(mid <= 0, lax.rem(mid + 2 * SLOTS, 2) == 1)
        near = jnp.where(to_first, near_first, near_second)
        near_slot = jnp.where(to_first, (mid + 1) // 2, mid // 2 - 1)
        rel = jnp.where(step < SLOTS, DIAG, jnp.where(in_mid, near, HERE))
        slot = jnp.where(step < SLOTS, step, jnp.where(in_mid, near_slot, step - 3 * SLOTS + 1))
        return rel, slot

    def dest_xy(rel):
        flip_x = jnp.where(rel <= ALONG_X, 1, 0)
        flip_y = jnp.where(lax.rem(rel, 2) == 0, 1, 0)
        xx = x + flip_x - 2 * flip_x * x
        yy = y + flip_y - 2 * flip_y * y
        return xx, yy

    def exists(rel, slot):
        _, yy = dest_xy(rel)
        return jnp.logical_or(slot < SLOTS - 1, yy == 0)

    def held(ref, slot):
        return ref.at[pl.ds(pl.multiple_of(slot * ROWS, ROWS), ROWS)]

    def total_of(rel, slot):
        return held(acc, rel * SLOTS + slot)

    def dot(left, left_rows, right, right_rows, cols=slice(None)):
        return lax.dot_general(a_buf[pl.ds(left, left_rows), cols], a_buf[pl.ds(right, right_rows), cols],
                               (((1,), (1,)), ((), ())), preferred_element_type=jnp.float32)

    def block_rows(rel, slot, kk):
        xx, yy = dest_xy(rel)
        p = device(xx, yy, kk)
        q = lax.rem(p - slot + GROUPS, GROUPS)
        hi = pl.multiple_of(jnp.maximum(p, q) * BLK, BLK)
        lo = pl.multiple_of(jnp.minimum(p, q) * BLK, BLK)
        return hi, lo

    def product(block, hi, lo, first=0, count=3):
        val = dot(hi, BLK, lo + first * STRIP, count * STRIP)
        for m in range(count):
            block[rows_of(first + m, 0, BLK)] = val[:, m * STRIP:(m + 1) * STRIP]

    def alone(work):
        def run(_, carry):
            work()
            return carry

        lax.fori_loop(0, one, run, 0)

    def pair_copy(src, dst, recv):
        return pltpu.make_async_remote_copy(
            src_ref=src, dst_ref=dst, send_sem=stage_sem, recv_sem=pair_sem.at[recv],
            device_id={'dp': pair}, device_id_type=MESH)

    def pair_block(step):
        return pair_copy(stage, total_of(*step_task(step)), 3 + lax.rem(step + 1, 3))

    def by_y(slot, m, first, dest_x, dest_y):
        if first:
            return (core if m == 0 else 1 - core) == 1

        def listed(*bits):
            return jnp.where(slot == 1, bits[0], jnp.where(slot == 2, bits[1], jnp.where(slot == 3, bits[2], bits[3])))

        to_zero = jnp.where(core == 0, listed(13, 2, 1, 1), listed(1, 1, 2, 2))
        to_one = jnp.where(core == 0, listed(5, 2, 1, 4), listed(5, 1, 2, 2))
        bits = jnp.where(dest_y == 1, 13, jnp.where(dest_x == 0, to_zero, to_one))
        return lax.rem(bits // 2 ** m, 2) == 1

    def relay_wait(slot, first, relay, sem, flags):
        each = [part_rows for _, part_rows in (FIRST_PARTS if first else PARTS)]
        rows = sum(jnp.where(flag, part_rows, 0) for flag, part_rows in zip(flags, each))
        possible = {sum(chosen) for n in range(1, len(each) + 1) for chosen in itertools.combinations(each, n)}
        for count in sorted(possible):
            @pl.when(rows == count)
            def _(count=count):
                whole = held(relay, slot).at[pl.ds(0, count)]
                pltpu.make_async_copy(whole, whole, sem.at[slot]).wait()

    def far_send(slot, m, first, along_y):
        return pltpu.make_async_remote_copy(
            src_ref=part(total_of(DIAG, slot), m, first),
            dst_ref=part(held(relay_x if along_y else relay_y, slot), m, first),
            send_sem=send_sem,
            recv_sem=(rx_sem if along_y else ry_sem).at[slot],
            device_id={'dp': nbr_y if along_y else nbr_x}, device_id_type=MESH)

    def near_send(rel, slot, m, first):
        along_y = rel == ALONG_Y
        return pltpu.make_async_remote_copy(
            src_ref=part(total_of(rel, slot), m, first),
            dst_ref=part(held(from_y if along_y else from_x, slot), m, first),
            send_sem=send_sem,
            recv_sem=from_sem.at[slot + jnp.where(slot == SLOTS - 1, m, 0)],
            device_id={'dp': nbr_y if along_y else nbr_x}, device_id_type=MESH)

    def finish_far(slot, m, first):
        total = part(total_of(DIAG, slot), m, first)
        total[...] = total[...] + part(mine, m, first)[...]
        along_y = by_y(slot, m, first, 1 - x, 1 - y)

        @pl.when(along_y)
        def _():
            far_send(slot, m, first, True).start()

        @pl.when(jnp.logical_not(along_y))
        def _():
            far_send(slot, m, first, False).start()

    def finish_near(rel, slot, first):
        if rel == ALONG_X:
            relay, sem = relay_x, rx_sem
            flags = [by_y(slot, m, first, 1 - x, y) for m in parts(first)]
        else:
            relay, sem = relay_y, ry_sem
            flags = [jnp.logical_not(by_y(slot, m, first, x, 1 - y)) for m in parts(first)]
        relay_wait(slot, first, relay, sem, flags)
        for m in parts(first):
            total = part(total_of(rel, slot), m, first)

            @pl.when(flags[m])
            def _(m=m, total=total):
                total[...] = total[...] + part(mine, m, first)[...] + part(held(relay, slot), m, first)[...]

            @pl.when(jnp.logical_not(flags[m]))
            def _(m=m, total=total):
                total[...] = total[...] + part(mine, m, first)[...]

            near_send(rel, slot, m, first).start()

    def finish(rel, slot, first):
        @pl.when(rel == DIAG)
        def _():
            for m in parts(first):
                finish_far(slot, m, first)

        for near in (ALONG_X, ALONG_Y):
            @pl.when(rel == near)
            def _(near=near):
                finish_near(near, slot, first)

        @pl.when(rel == HERE)
        def _():
            for m in parts(first):
                total = part(total_of(HERE, slot), m, first)
                total[...] = total[...] + part(mine, m, first)[...]

    def left_half(block, kk, h):
        row = pl.multiple_of((far + kk) * BLK, BLK)
        val = dot(row, BLK, row, 2 * STRIP, pl.ds(pl.multiple_of(h * half, half), half))
        for m in range(2):
            block[rows_of(m, 0, BLK)] = (
                jnp.where(h > 0, block[rows_of(m, 0, BLK)], 0.0) + val[:, m * STRIP:(m + 1) * STRIP])

    def left_product(block, kk):
        row = pl.multiple_of((far + kk) * BLK, BLK)
        val = dot(row, BLK, row, 2 * STRIP)
        for m in range(2):
            block[rows_of(m, 0, BLK)] = val[:, m * STRIP:(m + 1) * STRIP]

    def corner_product(block, kk):
        row = pl.multiple_of((far + kk) * BLK + 2 * STRIP, STRIP)
        block[rows_of(2, 2 * STRIP, BLK)] = dot(row, STRIP, row, STRIP)

    def first_half(h, carry):
        load_half(h).wait()
        left_half(stage, 1 - core, h)
        return carry

    two, last = pl.ds(0, 2 * BLK), pl.ds(2 * BLK, BLK)
    first_total, next_total = total_of(DIAG, 0), total_of(DIAG, 1)
    copies = (
        pair_copy(part(stage, 0, True), part(first_total, 0, True), 0),
        pair_copy(part(stage, 1, True), part(first_total, 1, True), 1),
        pair_copy(part(stage, 2, True), part(first_total, 2, True), 2),
        pair_copy(stage_next.at[two], next_total.at[two], 4),
        pair_copy(stage_next.at[last], next_total.at[last], 5),
    )

    lax.fori_loop(0, 2 * one, first_half, 0)
    pack_left(stage)
    pl.semaphore_wait(barrier, 3)
    copies[0].start()
    copies[1].start()
    load(1).wait()
    alone(lambda: left_product(mine, core))
    pack_left(mine)
    copies[0].wait_recv()
    finish_far(0, 0, True)
    copies[1].wait_recv()
    finish_far(0, 1, True)
    alone(lambda: corner_product(stage, 1 - core))
    pack_corner(stage)
    copies[2].start()
    load(2).wait()
    alone(lambda: product(stage_next, *block_rows(DIAG, 1, 1 - core), 0, 2))
    copies[3].start()
    alone(lambda: corner_product(mine, core))
    pack_corner(mine)
    copies[2].wait_recv()
    finish_far(0, 2, True)
    alone(lambda: product(mine, *block_rows(DIAG, 1, core), 0, 2))
    copies[3].wait_recv()
    finish_far(1, 0, False)
    finish_far(1, 1, False)
    alone(lambda: product(stage_next, *block_rows(DIAG, 1, 1 - core), 2, 1))
    copies[4].start()
    alone(lambda: product(mine, *block_rows(DIAG, 1, core), 2, 1))
    copies[4].wait_recv()
    finish_far(1, 2, False)
    finish_far(1, 3, False)
    both = acc.at[pl.ds(0, size(True) + ROWS)]
    pltpu.make_async_copy(both, both, stage_sem).wait()

    def body(step, carry):
        @pl.when(step == 2)
        def _():
            rest = pl.ds(0, (GROUPS - 3) * BLK)
            pltpu.make_async_copy(a_hbm.at[rest, :], a_buf.at[rest, :], load_sem.at[3]).wait()

        rel, slot = step_task(step)

        @pl.when(exists(rel, slot))
        def _():
            product(stage, *block_rows(rel, slot, 1 - core))

            @pl.when(slot == 0)
            def _():
                pack_left(stage)
                pack_corner(stage)

            pair_block(step).start()
            product(mine, *block_rows(rel, slot, core))

            @pl.when(slot == 0)
            def _():
                pack_left(mine)
                pack_corner(mine)
                pair_block(step).wait_recv()
                finish(rel, slot, True)

            @pl.when(slot > 0)
            def _():
                pair_block(step).wait_recv()
                finish(rel, slot, False)

            pair_block(step).wait_send()

        return carry

    lax.fori_loop(2, STEPS, body, 0)

    def arrived(slot):
        first = slot == 0
        two_of = acc.at[pl.ds(0, 2 * size(first))]
        pltpu.make_async_copy(two_of, two_of, from_sem.at[slot]).wait()
        for m in range(3):
            rows = pl.ds(*FIRST_PARTS[m]) if first else pl.ds(m * BLK, BLK)
            yield held(from_x, slot)[rows] + held(from_y, slot)[rows] + total_of(HERE, slot)[rows]

    unpack_symmetric(out_ref.at[0, 0], *arrived(0))
    for slot in range(1, SLOTS - 1):
        @pl.when(exists(HERE, slot))
        def _(slot=slot):
            for m, total in enumerate(arrived(slot)):
                out_ref[0, slot, :, m * STRIP:(m + 1) * STRIP] = total

    @pl.when(exists(HERE, SLOTS - 1))
    def _():
        for m, (start, count) in enumerate(PARTS):
            two_of = acc.at[pl.ds(0, 2 * count)]
            pltpu.make_async_copy(two_of, two_of, from_sem.at[SLOTS - 1 + m]).wait()
            rows = pl.ds(start, count)
            column, row = start // BLK, start % BLK
            out_ref[0, SLOTS - 1, row:row + count, column * STRIP:(column + 1) * STRIP] = (
                held(from_x, SLOTS - 1)[rows] + held(from_y, SLOTS - 1)[rows] + total_of(HERE, SLOTS - 1)[rows])

    @pl.when(jnp.logical_not(exists(HERE, SLOTS - 1)))
    def _():
        out_ref[0, SLOTS - 1] = jnp.zeros((BLK, BLK), jnp.float32)

    for longer in (1, 2):
        @pl.when(y == longer - 1)
        def _(longer=longer):
            everything = acc.at[pl.ds(0, 3 * size(True) + (3 * (SLOTS - 2) + longer) * ROWS)]
            pltpu.make_async_copy(everything, everything, send_sem).wait()


def solution(mesh):
    def local_gram(a_local):
        dma = pltpu.SemaphoreType.DMA

        def blocks(n):
            return pltpu.VMEM((n * ROWS, STRIP), jnp.float32)

        return pl.pallas_call(
            gram_kernel,
            out_shape=pltpu.VMEM((1, SLOTS, BLK, BLK), jnp.float32),
            in_specs=[pl.BlockSpec(memory_space=pl.ANY)],
            out_specs=pl.BlockSpec(memory_space=pltpu.VMEM),
            scratch_shapes=[
                pltpu.VMEM(a_local.shape, a_local.dtype),
                blocks(4 * SLOTS), blocks(1), blocks(1), blocks(1),
                blocks(SLOTS), blocks(SLOTS), blocks(SLOTS), blocks(SLOTS),
                dma((5,)), dma, dma((6,)), dma, dma((SLOTS + 3,)), dma((SLOTS,)), dma((SLOTS,)),
            ],
            compiler_params=pltpu.CompilerParams(
                collective_id=0, has_side_effects=True, vmem_limit_bytes=56623104),
        )(a_local)

    return jax.shard_map(local_gram, mesh=mesh, in_specs=(P('mat', 'dp'),), out_specs=P(('mat', 'dp')), check_vma=False)
```
